256 devices in a mesh: grp: 2 (over z_hi), gy: 4 (over z_lo), gz: 32 (over x, y, core).
Axes of the slice: x: 4, y: 4, z: 8 (z_hi: 2, z_lo: 4; z = z_hi * 4 + z_lo), core: 2. Of those that a mesh axis runs over, the one named last changes fastest.
Arguments:
- vorticity: float32 [2, 3, 256, 256, 256], P('grp', None, 'gz', 'gy'), may hold values from -6 to 6
- wind: float32 [2, 3], P('grp'), may hold values from 0.5 to 1.2
Outputs:
- new_vorticity: float32 [2, 3, 256, 256, 256], P('grp', None, 'gz', 'gy')
- velocity: float32 [2, 3, 256, 256, 256], P('grp', None, 'gz', 'gy')
The draws below stay inside these ranges and needn't reach their ends.
All inputs are finite; a program needn't handle non-finite values.
Results may differ from the reference program's by a relative error of at most 0.0003.
Values sent between devices are 32-bit elements; how exact they have to be, the bound alone decides.
No kernel may reach another device: no remote copies, remote signals or barrier semaphores. Data moves between devices by JAX's collectives and lax.ppermute only.
A program may use at most 128 MiB of HBM per device.

```python
import math
import jax
import jax.numpy as jnp

NX = 256
NY = 256
NZ = 256


def draw_vorticity(key, part):
    shape = (2, 3, NZ, NY, NX)
    first = jax.random.fold_in(key, 0)
    return jnp.clip(jax.random.normal(first, shape, jnp.float32), -6.0, 6.0)


def shard_levels(key, shape, cuts, smallest, largest):
    def one(position, parts):
        steps = jax.random.uniform(jax.random.fold_in(jax.random.fold_in(key, 6), position), (parts,), jnp.float32, smallest / len(cuts), largest / len(cuts))
        return jnp.repeat(jnp.exp(steps), shape[position] // parts).reshape((-1,) + (1,) * (len(shape) - position - 1))

    gain = one(*cuts[0])
    for cut in cuts[1:]:
        gain = gain * one(*cut)
    return gain


def setup_inputs(seed: int = 0) -> dict:
    key_of = jax.random.split(jax.random.key(seed), 3)
    vorticity = draw_vorticity(jax.random.fold_in(key_of[2], 71), 0)
    wind = jnp.clip(0.5 + 0.70000005 * jax.random.uniform(key_of[1], (2, 3), jnp.float32) ** shard_levels(key_of[1], (2, 3), ((0, 2),), -0.2, 0.2), 0.5, 1.2)
    return dict(vorticity=vorticity, wind=wind)


TIME_STEP = 0.4


def kernel_weight(offset):
    mag = jnp.abs(offset)
    inner = 1.0 - 2.5 * mag * mag + 1.5 * mag * mag * mag
    outer = 0.5 * (2.0 - mag) * (2.0 - mag) * (1.0 - mag)
    return jnp.where(mag < 1.0, inner, jnp.where(mag < 2.0, outer, 0.0 * mag))


def wave_numbers(count):
    index = jnp.arange(count, dtype=jnp.int32)
    signed = jnp.where(index < count // 2, index, index - count)
    return signed.astype(jnp.float32) * (2.0 * math.pi / count)


def velocity_of(field, drift):
    spectrum = jnp.fft.fftn(field, axes=(1, 2, 3))
    wave_z = wave_numbers(NZ)[:, None, None]
    wave_y = wave_numbers(NY)[None, :, None]
    wave_x = wave_numbers(NX)[None, None, :]
    squared = wave_x * wave_x + wave_y * wave_y + wave_z * wave_z
    inverse = jnp.where(squared > 0, 1.0 / jnp.where(squared > 0, squared, 1.0), 0.0 * squared)
    stream = spectrum * inverse
    cross_x = wave_y * stream[2] - wave_z * stream[1]
    cross_y = wave_z * stream[0] - wave_x * stream[2]
    cross_z = wave_x * stream[1] - wave_y * stream[0]
    result = jnp.real(jnp.fft.ifftn(1j * jnp.stack([cross_x, cross_y, cross_z]), axes=(1, 2, 3)))
    return result + drift[:, None, None, None]


def central(values, axis):
    return (jnp.roll(values, -1, axis) - jnp.roll(values, 1, axis)) * 0.5


def stretch(field, speed, grad_x):
    grad_y = central(speed, 2)
    grad_z = central(speed, 1)
    return field + TIME_STEP * (field[0:1] * grad_x + field[1:2] * grad_y + field[2:3] * grad_z)


def remesh_periodic(values, shift, axis):
    total = jnp.zeros_like(values)
    for offset in range(-2, 3):
        total = total + jnp.roll(values, offset, axis) * kernel_weight(offset - jnp.roll(shift, offset, axis))
    return total


def remesh_inflow(values, shift, ghost_values, ghost_shift):
    q_ext = jnp.concatenate([ghost_values, values, jnp.zeros_like(values[..., :2])], -1)
    d_ext = jnp.concatenate([ghost_shift, shift, jnp.zeros_like(shift[..., :2])], -1)
    total = jnp.zeros_like(values)
    for offset in range(-2, 3):
        start = 2 - offset
        total = total + q_ext[..., start:start + NX] * kernel_weight(offset - d_ext[..., start:start + NX])
    return total


def reference(vorticity, wind):
    speed_pre = velocity_of(vorticity[0], wind[0])
    speed_wake = velocity_of(vorticity[1], wind[1])
    strength_pre = stretch(vorticity[0], speed_pre, central(speed_pre, 3))
    extended = jnp.concatenate([speed_pre[..., NX - 1:], speed_wake, speed_wake[..., NX - 1:]], -1)
    grad_wake = (extended[..., 2:] - extended[..., :-2]) * 0.5
    strength_wake = stretch(vorticity[1], speed_wake, grad_wake)
    moved_pre = remesh_periodic(strength_pre, TIME_STEP * speed_pre[0:1], 3)
    moved_wake = remesh_inflow(strength_wake, TIME_STEP * speed_wake[0:1], strength_pre[..., NX - 2:], TIME_STEP * speed_pre[0:1][..., NX - 2:])
    outputs = []
    for moved, speed in ((moved_pre, speed_pre), (moved_wake, speed_wake)):
        lateral = remesh_periodic(moved, TIME_STEP * speed[1:2], 2)
        outputs.append(remesh_periodic(lateral, TIME_STEP * speed[2:3], 1))
    return jnp.stack(outputs), jnp.stack([speed_pre, speed_wake])
```

```python
import math

import jax
import jax.numpy as jnp
import numpy as np
from jax import lax
from jax.experimental import pallas as pl
from jax.experimental.pallas import tpu as pltpu
from jax.sharding import PartitionSpec as P

TIME_STEP = 0.4
BF16 = jnp.bfloat16
F32 = jnp.float32
VMEM_LIMIT = 60 * 1024 * 1024


def angles(count):
    index = np.arange(count)
    return (index[:, None] * index[None, :] % count) * (2.0 * math.pi / count)


def halves(table):
    table = np.asarray(table, np.float32)
    high = table.astype(BF16)
    low = (table - high.astype(np.float32)).astype(BF16)
    return high, low


def left_table(table):
    high, low = halves(table)
    return np.concatenate([high, high, low], 1)


def right_table(table):
    high, low = halves(table)
    return np.concatenate([high, high, low], 0)


def split(value):
    high = value.astype(BF16)
    low = (value - high.astype(F32)).astype(BF16)
    return high, low


def streamwise_tables(count):
    half = count // 2
    cosine, sine = np.cos(angles(count)), np.sin(angles(count))
    alternate = 1.0 - 2.0 * (np.arange(count) % 2)
    forward = np.concatenate([cosine[:half], alternate[None], -sine[1:half]], 0)
    scale = np.full((half, 1), 2.0)
    scale[0] = 1.0
    backward = np.concatenate([scale * cosine[:half], alternate[None], -2.0 * sine[1:half]], 0)
    return forward, backward / count


def vertical_table(count, blocks):
    local = count // blocks
    z = np.arange(blocks)[None, :, None] * local + np.arange(local // 2)[None, None, :] * 2
    z = z + np.arange(2)[:, None, None]
    phase = (np.arange(count)[:, None, None, None] * z[None] % count) * (2.0 * math.pi / count)
    cosine, sine = np.cos(phase), np.sin(phase)
    real = np.stack([cosine, sine], 3)
    imag = np.stack([-sine, cosine], 3)
    return np.stack([real, imag]).reshape(2 * count, 2 * count)


def streamwise_forward(field_ref, table_ref, out_ref):
    comps, local_z, local_y, count = field_ref.shape
    rows = local_z * local_y
    table = table_ref[...]
    for c in range(comps):
        value = field_ref[c].reshape(rows, count)
        high, low = split(value)
        stacked = jnp.concatenate([high, low, high], 1)
        result = lax.dot_general(
            table, stacked, (((1,), (1,)), ((), ())), preferred_element_type=F32
        )
        for part in range(2):
            for k in range(0, count // 2, 8):
                for a in range(rows // 128):
                    top = part * (count // 2) + k
                    out_ref[pl.ds(k * 24 + c * 8 + part * 4 + a, 8, stride=24), :] = result[
                        top : top + 8, a * 128 : (a + 1) * 128
                    ]


def product(left, right):
    return jnp.dot(left, right, preferred_element_type=F32)


def left_product(table, value):
    high, low = split(value)
    return product(table, jnp.concatenate([high, low, high], 0))


def right_product(value, table):
    high, low = split(value)
    return product(jnp.concatenate([high, low, high], 1), table)


def signed_waves(index, count, odd):
    signed = jnp.where(index < count // 2, index, index - count)
    if odd:
        signed = jnp.where(index == count // 2, 0, signed)
    return signed.astype(F32) * (2.0 * math.pi / count)


def plane_kernel(owner_ref, in_ref, z_ref, y_ref, back_ref, flip_ref, out_ref, plain_ref):
    n = y_ref.shape[1] // 2
    owner = owner_ref[0]
    is_packed = owner == 0
    low_lanes = lax.broadcasted_iota(jnp.int32, (n, 128), 1) < 64
    row = lax.broadcasted_iota(jnp.int32, (n, n), 0)
    col = lax.broadcasted_iota(jnp.int32, (n, n), 1)
    wave_x = owner.astype(F32) * (2.0 * math.pi / n)
    wave_z = signed_waves(row, n, False)
    wave_y = signed_waves(col, n, False)
    curl_z = signed_waves(row, n, True)
    curl_y = signed_waves(col, n, True)
    plane = wave_y * wave_y + wave_z * wave_z
    squared = plane + wave_x * wave_x
    scale = jnp.where(squared > 0, 1.0 / jnp.where(squared > 0, squared, 1.0), 0.0)
    top_scale = 1.0 / (plane + math.pi * math.pi)
    sigma = jnp.where(is_packed, 0.5 * (scale + top_scale), scale)
    delta = 0.5 * (scale - top_scale)
    for c in range(3):
        blocks = [
            in_ref[32 * g : 32 * g + 32, 8 * c : 8 * c + 8, :].reshape(n, 128) for g in range(4)
        ]
        tops, bottoms = [], []
        for g in (0, 2):
            first, second = blocks[g], blocks[g + 1]
            tops.append(jnp.where(low_lanes, first, pltpu.roll(second, 64, 1)))
            bottoms.append(jnp.where(low_lanes, pltpu.roll(first, 64, 1), second))
        value = jnp.concatenate(
            [jnp.concatenate(tops, 1), jnp.concatenate(bottoms, 1)], 0
        )
        value = left_product(z_ref[...], value)
        value = right_product(value, y_ref[...])
        real_cos, real_sin = value[:n, :n], value[:n, n:]
        imag_cos, imag_sin = value[n:, :n], value[n:, n:]
        plain_ref[c, :n, :] = (real_cos + imag_sin) * sigma
        plain_ref[c, n:, :] = (imag_cos - real_sin) * sigma

        @pl.when(is_packed)
        def _():
            turned = jnp.concatenate([real_cos - imag_sin, imag_cos + real_sin], 1)
            high, low = split(turned)
            mirror = product(flip_ref[...], high) + product(flip_ref[...], low)
            plain_ref[c, :n, :] += mirror[:, :n] * delta
            plain_ref[c, n:, :] -= mirror[:, n:] * delta

    for c in range(3):
        if c == 0:
            def cross(part):
                return curl_y * plain_ref[2, part] - curl_z * plain_ref[1, part]
        elif c == 1:
            def cross(part):
                return curl_z * plain_ref[0, part] - wave_x * plain_ref[2, part]
        else:
            def cross(part):
                return wave_x * plain_ref[1, part] - curl_y * plain_ref[0, part]
        value = jnp.concatenate([-cross(slice(n, 2 * n)), cross(slice(0, n))], 0)
        value = right_product(value, y_ref[...])
        real = value[:n, :n] - value[n:, n:]
        imag = value[n:, :n] + value[:n, n:]
        value = left_product(back_ref[...], jnp.concatenate([real, imag], 0))
        for pair in range(2):
            top = value[:n, 128 * pair : 128 * pair + 128]
            bottom = value[n:, 128 * pair : 128 * pair + 128]
            first = jnp.where(low_lanes, top, pltpu.roll(bottom, 64, 1))
            second = jnp.where(low_lanes, pltpu.roll(top, 64, 1), bottom)
            for g, block in ((2 * pair, first), (2 * pair + 1, second)):
                out_ref[32 * g : 32 * g + 32, 8 * c : 8 * c + 8, :] = block.reshape(32, 8, 128)


def streamwise_backward(in_ref, table_ref, drift_ref, out_ref):
    comps, local_z, local_y, count = out_ref.shape
    for c in range(comps):
        parts = []
        for part in range(2):
            chunks = [
                in_ref[pl.ds(c * 8 + part * 4 + a, count // 2, stride=24), :] for a in range(4)
            ]
            parts.append(jnp.concatenate(chunks, 1))
        value = jnp.concatenate(parts, 0).T
        result = right_product(value, table_ref[...]) + drift_ref[0, c]
        out_ref[c] = result.reshape(local_z, local_y, count)


def call(kernel, shape, args, smem=(), scratch=()):
    specs = [
        pl.BlockSpec(memory_space=pltpu.SMEM if i in smem else pltpu.VMEM)
        for i in range(len(args))
    ]
    return pl.pallas_call(
        kernel,
        out_shape=jax.ShapeDtypeStruct(shape, F32),
        in_specs=specs,
        out_specs=pl.BlockSpec(memory_space=pltpu.VMEM),
        scratch_shapes=list(scratch),
        compiler_params=pltpu.CompilerParams(vmem_limit_bytes=VMEM_LIMIT),
    )(*args)


def forward_lines(field):
    count = field.shape[3]
    forward, _ = streamwise_tables(count)
    table = jnp.asarray(left_table(forward))
    return call(streamwise_forward, (count // 2 * 24, 128), (field, table))


def solve_plane(spectrum, owner, count, blocks):
    vertical = vertical_table(count, blocks)
    phase = angles(count)
    lateral = np.concatenate([np.cos(phase), np.sin(phase)], 1)
    flip = np.zeros((count, count), np.float32)
    flip[np.arange(count), -np.arange(count) % count] = 1.0
    args = (
        owner.reshape(1),
        spectrum,
        jnp.asarray(left_table(vertical)),
        jnp.asarray(right_table(lateral)),
        jnp.asarray(left_table(vertical.T / (count * count))),
        jnp.asarray(flip.astype(BF16)),
    )
    scratch = (pltpu.VMEM((3, 2 * count, count), F32),)
    return call(plane_kernel, spectrum.shape, args, smem=(0,), scratch=scratch)


def backward_lines(spectrum, drift, shape):
    _, backward = streamwise_tables(shape[3])
    table = jnp.asarray(right_table(backward))
    return call(streamwise_backward, shape, (spectrum, table, drift), smem=(2,))


def shifted(value, axis, steps):
    count = lax.axis_size(axis)
    initial, last = (max(0, -steps), min(count, count - steps))
    return lax.ppermute(value, axis, [(source, source + steps) for source in range(initial, last)])


def padded(array, sides, width):
    edges = {}
    for axis, dim in sides:
        devices, length = (lax.axis_size(axis), array.shape[dim])
        up = [(i, (i + 1) % devices) for i in range(devices)]
        last = lax.slice_in_dim(array, length - width, length, axis=dim)
        initial = lax.slice_in_dim(array, 0, width, axis=dim)
        edges[dim] = (
            lax.ppermute(last, axis, up),
            lax.ppermute(initial, axis, [(b, a) for a, b in up]),
        )
    done = []
    for _, dim in sides:
        low, high = edges[dim]
        around = [(width, width) if d in done else (0, 0) for d in range(array.ndim)]
        array = jnp.concatenate([jnp.pad(low, around), array, jnp.pad(high, around)], axis=dim)
        done.append(dim)
    return array


def extended_2(cells, sides, width):
    for axis, dim in sides:
        count = lax.axis_size(axis)
        head = lax.slice_in_dim(cells, 0, width, axis=dim)
        tail = lax.slice_in_dim(cells, cells.shape[dim] - width, cells.shape[dim], axis=dim)
        cells = jnp.concatenate(
            [
                lax.ppermute(tail, axis, [(i, (i + 1) % count) for i in range(count)]),
                cells,
                lax.ppermute(head, axis, [((i + 1) % count, i) for i in range(count)]),
            ],
            axis=dim,
        )
    return cells


def kernel_weight(offset):
    mag = jnp.abs(offset)
    inner = 1.0 - 2.5 * mag * mag + 1.5 * mag * mag * mag
    outer = 0.5 * (2.0 - mag) * (2.0 - mag) * (1.0 - mag)
    return jnp.where(mag < 1.0, inner, jnp.where(mag < 2.0, outer, 0.0 * mag))


def body(vorticity, wind):
    is_wake = lax.axis_index("grp") == 1
    field = vorticity[0]
    count_x = field.shape[3]
    size_gz = lax.axis_size("gz")
    groups = lax.axis_size("gy") * size_gz
    owner = lax.axis_index("gy") * size_gz + lax.axis_index("gz")
    axes = ("gy", "gz")
    spectrum = forward_lines(field).reshape(groups, 24, 128)
    spectrum = lax.all_to_all(spectrum, axes, split_axis=0, concat_axis=0, tiled=True)
    spectrum = solve_plane(spectrum, owner, count_x, size_gz)
    spectrum = lax.all_to_all(spectrum, axes, split_axis=0, concat_axis=0, tiled=True)
    velocity = backward_lines(spectrum.reshape(groups * 24, 128), wind, field.shape)
    planes = shifted(velocity[..., count_x - 2 :], "grp", 1)
    rimmed = padded(velocity, (("gz", 1), ("gy", 2)), 1)
    grad_z = (rimmed[:, 2:, 1:-1, :] - rimmed[:, :-2, 1:-1, :]) * 0.5
    grad_y = (rimmed[:, 1:-1, 2:, :] - rimmed[:, 1:-1, :-2, :]) * 0.5
    left_side = jnp.where(is_wake, planes[..., 1:], velocity[..., count_x - 1 :])
    right_side = jnp.where(is_wake, velocity[..., count_x - 1 :], velocity[..., :1])
    extended = jnp.concatenate([left_side, velocity, right_side], -1)
    grad_x = (extended[..., 2:] - extended[..., :-2]) * 0.5
    strength = field + TIME_STEP * (field[0:1] * grad_x + field[1:2] * grad_y + field[2:3] * grad_z)
    ghost = shifted(strength[..., count_x - 2 :], "grp", 1)
    shift_x = TIME_STEP * velocity[0]
    left_q = jnp.where(is_wake, ghost, strength[..., count_x - 2 :])
    left_d = jnp.where(is_wake, TIME_STEP * planes[0], shift_x[..., count_x - 2 :])
    right_q = jnp.where(is_wake, 0.0, strength[..., :2])
    right_d = jnp.where(is_wake, 0.0, shift_x[..., :2])
    q_ext = jnp.concatenate([left_q, strength, right_q], -1)
    d_ext = jnp.concatenate([left_d, shift_x, right_d], -1)
    moved = jnp.zeros_like(strength)
    for offset in range(-2, 3):
        start = 2 - offset
        moved = moved + q_ext[..., start : start + count_x] * kernel_weight(
            offset - d_ext[..., start : start + count_x]
        )
    packed = jnp.concatenate([moved, TIME_STEP * velocity[1:2]], 0)
    rim_rows = extended_2(packed, (("gy", 2),), 2)
    width_y = moved.shape[2]
    lateral = jnp.zeros_like(moved)
    for offset in range(-2, 3):
        start = 2 - offset
        lateral = lateral + rim_rows[:3, :, start : start + width_y, :] * kernel_weight(
            offset - rim_rows[3:4, :, start : start + width_y, :]
        )
    packed = jnp.concatenate([lateral, TIME_STEP * velocity[2:3]], 0)
    rim_cols = extended_2(packed, (("gz", 1),), 2)
    width_z = moved.shape[1]
    result = jnp.zeros_like(moved)
    for offset in range(-2, 3):
        start = 2 - offset
        result = result + rim_cols[:3, start : start + width_z, :, :] * kernel_weight(
            offset - rim_cols[3:4, start : start + width_z, :, :]
        )
    return (result[None], velocity[None])


def solution(mesh):
    return jax.shard_map(
        body,
        mesh=mesh,
        in_specs=(P("grp", None, "gz", "gy", None), P("grp", None)),
        out_specs=(P("grp", None, "gz", "gy", None), P("grp", None, "gz", "gy", None)),
        check_vma=False,
    )
```

```python
import math

import jax
import jax.numpy as jnp
import numpy as np
from jax import lax
from jax.experimental import pallas as pl
from jax.experimental.pallas import tpu as pltpu
from jax.sharding import PartitionSpec as P

TIME_STEP = 0.4
RIM = 3
BF16 = jnp.bfloat16
F32 = jnp.float32


def forward_table(count):
    index = np.arange(count)
    phase = (index[:, None] * index[None, :] % count) * (2.0 * math.pi / count)
    half = count // 2
    alternate = 1.0 - 2.0 * (index % 2)
    table = np.concatenate([np.cos(phase[:half]), alternate[None], -np.sin(phase[1:half])], 0)
    table = table.astype(np.float32)
    high = table.astype(BF16)
    return np.stack([high, (table - high.astype(np.float32)).astype(BF16)])


def split(value):
    high = value.astype(BF16)
    low = (value - high.astype(F32)).astype(BF16)
    return high, low


def turns(product, count):
    phase = (product % count).astype(F32) * (2.0 * math.pi / count)
    return jnp.cos(phase), jnp.sin(phase)


def run_time_tables(start, count, blocks):
    def index(shape, dim):
        return lax.broadcasted_iota(jnp.int32, shape, dim) + start

    shape = (2 * count, 2 * count)
    row, col = index(shape, 0), index(shape, 1)
    local = count // blocks

    def place(i):
        return i % count // 8 * local + i % 4 * 2 + i // count

    def part(i):
        return i // 4 % 2

    cosine, sine = turns((row % count) * place(col), count)
    vertical = jnp.where(
        row // count == part(col), cosine, jnp.where(row < count, sine, -sine)
    )
    cosine, sine = turns((col % count) * place(row), count)
    back = jnp.where(
        col // count == part(row), cosine, jnp.where(col < count, sine, -sine)
    ) * (1.0 / (count * count))
    shape = (count, 2 * count)
    cosine, sine = turns(index(shape, 0) * (index(shape, 1) % count), count)
    lateral = jnp.where(index(shape, 1) < count, cosine, sine)
    shape = (count, count)
    row, col = index(shape, 0), index(shape, 1)
    flip = ((row + col) % count == 0).astype(BF16)
    half = count // 2
    cosine, sine = turns((row % half) * col, count)
    alternate = (1 - 2 * (col % 2)).astype(F32)
    scale = jnp.where(row % half == 0, 1.0, 2.0) * (1.0 / count)
    streamwise = jnp.where(
        row < half, cosine * scale, jnp.where(row == half, alternate * scale, -sine * scale)
    )
    def tripled(table, axis):
        high = lax.reduce_precision(table, 8, 7)
        low = (table - high).astype(BF16)
        high = high.astype(BF16)
        return jnp.concatenate([high, high, low], axis)

    plane = (tripled(vertical, 1), tripled(lateral, 0), tripled(back, 1), flip)
    return plane, tripled(streamwise, 0)


def streamwise_forward(field_any, table_any, out_ref, field_ref, table_ref, sems):
    comps, local_z, local_y, count = field_ref.shape
    rows = local_z * local_y
    half = count // 2
    copies = [pltpu.make_async_copy(table_any, table_ref, sems.at[comps])]
    for c in range(comps):
        copies.append(pltpu.make_async_copy(field_any.at[c], field_ref.at[c], sems.at[c]))
    for copy in copies:
        copy.start()
    copies[0].wait()
    dims = (((1,), (1,)), ((), ()))
    for c in range(comps):
        copies[c + 1].wait()
        high, low = split(field_ref[c].reshape(rows, count))

        def term(i, value):
            return lax.dot_general(table_ref[i], value, dims, preferred_element_type=F32)

        result = term(0, high) + term(0, low) + term(1, high)
        for part in range(2):
            for k in range(0, half, 8):
                for a in range(rows // 128):
                    top = part * half + k
                    out_ref[pl.ds(k * 24 + c * 8 + part * 4 + a, 8, stride=24), :] = result[
                        top : top + 8, a * 128 : (a + 1) * 128
                    ]


def product(left, right):
    return jnp.dot(left, right, preferred_element_type=F32)


def left_product(table, value):
    high, low = split(value)
    return product(table, jnp.concatenate([high, low, high], 0))


def right_product(value, table):
    high, low = split(value)
    return product(jnp.concatenate([high, low, high], 1), table)


def signed_waves(index, count, odd):
    signed = jnp.where(index < count // 2, index, index - count)
    if odd:
        signed = jnp.where(index == count // 2, 0, signed)
    return signed.astype(F32) * (2.0 * math.pi / count)


def plane_kernel(
    owner_ref, in_ref, z_any, y_any, back_any, flip_any, out_ref,
    plain_ref, z_ref, y_ref, back_ref, flip_ref, sems,
):
    n = y_ref.shape[1] // 2
    pairs = ((z_any, z_ref), (y_any, y_ref), (back_any, back_ref), (flip_any, flip_ref))
    copies = [pltpu.make_async_copy(s, d, sems.at[i]) for i, (s, d) in enumerate(pairs)]
    for copy in copies:
        copy.start()
    owner = owner_ref[0]
    is_packed = owner == 0
    low_lanes = lax.broadcasted_iota(jnp.int32, (n, 128), 1) < 64
    row = lax.broadcasted_iota(jnp.int32, (n, n), 0)
    col = lax.broadcasted_iota(jnp.int32, (n, n), 1)
    wave_x = owner.astype(F32) * (2.0 * math.pi / n)
    wave_z = signed_waves(row, n, False)
    wave_y = signed_waves(col, n, False)
    curl_z = signed_waves(row, n, True)
    curl_y = signed_waves(col, n, True)
    plane = wave_y * wave_y + wave_z * wave_z
    squared = plane + wave_x * wave_x
    scale = jnp.where(squared > 0, 1.0 / jnp.where(squared > 0, squared, 1.0), 0.0)
    top_scale = 1.0 / (plane + math.pi * math.pi)
    sigma = jnp.where(is_packed, 0.5 * (scale + top_scale), scale)
    delta = 0.5 * (scale - top_scale)
    copies[0].wait()
    copies[1].wait()
    copies[3].wait()
    for c in range(3):
        blocks = [
            in_ref[32 * g : 32 * g + 32, 8 * c : 8 * c + 8, :].reshape(n, 128) for g in range(4)
        ]
        tops, bottoms = [], []
        for g in (0, 2):
            first, second = blocks[g], blocks[g + 1]
            tops.append(jnp.where(low_lanes, first, pltpu.roll(second, 64, 1)))
            bottoms.append(jnp.where(low_lanes, pltpu.roll(first, 64, 1), second))
        value = jnp.concatenate(
            [jnp.concatenate(tops, 1), jnp.concatenate(bottoms, 1)], 0
        )
        value = left_product(z_ref[...], value)
        value = right_product(value, y_ref[...])
        real_cos, real_sin = value[:n, :n], value[:n, n:]
        imag_cos, imag_sin = value[n:, :n], value[n:, n:]
        plain_ref[c, :n, :] = (real_cos + imag_sin) * sigma
        plain_ref[c, n:, :] = (imag_cos - real_sin) * sigma

        @pl.when(is_packed)
        def _():
            turned = jnp.concatenate([real_cos - imag_sin, imag_cos + real_sin], 1)
            high, low = split(turned)
            mirror = product(flip_ref[...], high) + product(flip_ref[...], low)
            plain_ref[c, :n, :] += mirror[:, :n] * delta
            plain_ref[c, n:, :] -= mirror[:, n:] * delta

    copies[2].wait()
    for c in range(3):
        if c == 0:
            def cross(part):
                return curl_y * plain_ref[2, part] - curl_z * plain_ref[1, part]
        elif c == 1:
            def cross(part):
                return curl_z * plain_ref[0, part] - wave_x * plain_ref[2, part]
        else:
            def cross(part):
                return wave_x * plain_ref[1, part] - curl_y * plain_ref[0, part]
        value = jnp.concatenate([-cross(slice(n, 2 * n)), cross(slice(0, n))], 0)
        value = right_product(value, y_ref[...])
        real = value[:n, :n] - value[n:, n:]
        imag = value[n:, :n] + value[:n, n:]
        value = left_product(back_ref[...], jnp.concatenate([real, imag], 0))
        for pair in range(2):
            top = value[:n, 128 * pair : 128 * pair + 128]
            bottom = value[n:, 128 * pair : 128 * pair + 128]
            first = jnp.where(low_lanes, top, pltpu.roll(bottom, 64, 1))
            second = jnp.where(low_lanes, pltpu.roll(top, 64, 1), bottom)
            for g, block in ((2 * pair, first), (2 * pair + 1, second)):
                out_ref[32 * g : 32 * g + 32, 8 * c : 8 * c + 8, :] = block.reshape(32, 8, 128)


def streamwise_backward(
    in_ref, table_ref, drift_ref, out_ref, speed_ref, low_ref, high_ref
):
    comps, local_z, local_y, count = out_ref.shape

    def component(c, carry):
        parts = []
        for part in range(2):
            chunks = [
                in_ref[pl.ds(c * 8 + part * 4 + a, count // 2, stride=24), :] for a in range(4)
            ]
            parts.append(jnp.concatenate(chunks, 1))
        value = jnp.concatenate(parts, 0).T
        result = right_product(value, table_ref[...]) + drift_ref[0, c]
        out_ref[c] = result.reshape(local_z, local_y, count)
        speed_ref[c] = result.reshape(local_z, local_y, count)
        return carry

    lax.fori_loop(0, comps, component, 0)
    for c in range(comps):
        for z in range(local_z):
            row = (c * local_z + z) * RIM
            low_ref[row : row + RIM, :] = out_ref[c, z, 0:RIM, :]
            high_ref[row : row + RIM, :] = out_ref[c, z, local_y - RIM : local_y, :]


def edge_kernel(speed_ref, above_ref, below_ref, tail_ref, up_ref, down_ref):
    comps, local_z, local_y, count = speed_ref.shape
    for c in range(comps):
        for z in range(local_z):
            row = (c * local_z + z) * RIM
            tail_ref[c, z, 0:RIM, :] = above_ref[row : row + RIM, :]
            tail_ref[c, z, RIM : 8 - RIM, :] = jnp.zeros((8 - 2 * RIM, count), F32)
            tail_ref[c, z, 8 - RIM : 8, :] = below_ref[row : row + RIM, :]
        for target, first in ((up_ref, local_z - RIM), (down_ref, 0)):
            for z in range(RIM):
                target[c, z, 0:local_y, :] = speed_ref[c, first + z]
                target[c, z, local_y : local_y + 8, :] = tail_ref[c, first + z]


def weights(shift, small=False):
    zero = jnp.zeros_like(shift)
    if small:
        left = shift < 0
        frac = jnp.where(left, shift + 1.0, shift)
    else:
        base = jnp.floor(shift)
        frac = shift - base
    rest = 1.0 - frac
    side = -0.5 * frac * rest
    before = side * rest
    after = side * frac
    near = 1.0 + frac * frac * (1.5 * frac - 2.5)
    far = 1.0 - (before + near + after)
    if small:
        values = [zero, before, near, far, after, zero]
        return {o: jnp.where(left, values[o + 3], values[o + 2]) for o in range(-2, 3)}
    at = {k: base == k for k in range(-4, 4)}
    result = {}
    for o in range(-2, 3):
        value = jnp.where(at[o - 2], after, zero)
        value = jnp.where(at[o - 1], far, value)
        value = jnp.where(at[o], near, value)
        result[o] = jnp.where(at[o + 1], before, value)
    return result


def rotated(value, steps):
    return pltpu.roll(value, steps % value.shape[1], 1)


def inflow_kernel(wake_ref, speed_ref, tail_ref, low_ref, high_ref, field_ref, out_ref, line_ref):
    planes, local_z = field_ref.shape[1], speed_ref.shape[1]
    lane = lax.broadcasted_iota(jnp.int32, (72, 128), 1)

    @pl.when(wake_ref[0] == 0)
    def _():
        line_ref[...] = jnp.zeros(line_ref.shape, F32)
        for q in range(planes + 2):
            columns = jnp.zeros((72, 128), F32)
            for c in range(3):
                if q < RIM:
                    first, last = low_ref[c, q, :, :128], low_ref[c, q, :, 128:]
                elif q < RIM + local_z:
                    z = q - RIM
                    pieces = [
                        jnp.concatenate([speed_ref[c, z, :, lanes], tail_ref[c, z, :, lanes]], 0)
                        for lanes in (slice(0, 128), slice(128, 256))
                    ]
                    first, last = pieces
                else:
                    z = q - RIM - local_z
                    first, last = high_ref[c, z, :, :128], high_ref[c, z, :, 128:]
                at = 4 * c
                here = (lane >= at) & (lane < at + 3)
                columns = jnp.where(here, rotated(last, at + 3), columns)
                columns = jnp.where(lane == at + 3, rotated(first, at + 3), columns)
                if 1 <= q <= planes:
                    at = 12 + 2 * c
                    here = (lane >= at) & (lane < at + 2)
                    columns = jnp.where(
                        here, rotated(field_ref[c, q - 1, :, 128:], at + 2), columns
                    )
            gap = jnp.zeros((40, 128), F32)
            whole = jnp.concatenate([columns, columns[:8], gap, columns[64:]], 0)
            line_ref[24 * q : 24 * q + 24, :] = whole.T[:24]

        def line(row, plane):
            return line_ref[pl.ds(24 * plane + row, 16, stride=24), :]

        shift = [weights(TIME_STEP * line(x, 1)) for x in (1, 2)]
        part = [[line(12 + 2 * c + x, 1) for x in range(2)] for c in range(3)]
        for c in range(3):
            strength = []
            for x in range(2):
                row = 4 * c + 1 + x
                value = line(row, 1)
                strength.append(
                    part[c][x]
                    + (0.5 * TIME_STEP)
                    * (
                        part[0][x] * (line(row + 1, 1) - line(row - 1, 1))
                        + part[1][x] * (rotated(value, -1) - rotated(value, 1))
                        + part[2][x] * (line(row, 2) - line(row, 0))
                    )
                )
            rows = (
                strength[0] * shift[0][2] + strength[1] * shift[1][1],
                strength[1] * shift[1][2],
                line(4 * c + 2, 1),
            )
            for i, row in enumerate(rows):
                out_ref[pl.ds(4 * c + i, 16, stride=16), :] = row


def fill_speed(speed_ref, tail_ref, low_ref, high_ref, all_ref):
    local_z = speed_ref.shape[1]
    most = jnp.zeros((8, 128), F32)
    for c in range(3):
        for t in range(2):
            lanes = slice(128 * t, 128 * t + 128)
            for own, end, row, first in (
                (low_ref, low_ref, 64, 0),
                (speed_ref, tail_ref, 0, RIM),
                (high_ref, high_ref, 64, RIM + local_z),
            ):
                planes = slice(first, first + own.shape[1])
                body = own[c, :, 0:64, lanes]
                tail = end[c, :, row : row + 8, lanes]
                all_ref[c, planes, t, 8:72, :] = body
                all_ref[c, planes, t, 0:8, :] = tail
                all_ref[c, planes, t, 72:80, :] = tail
                all_ref[c, planes, t, 80:88, :] = body[:, 0:8]
                most = jnp.maximum(most, jnp.max(jnp.abs(body).reshape(-1, 8, 128), 0))
                most = jnp.maximum(most, jnp.max(jnp.abs(tail), 0))
    return jnp.max(most)


def wake_kernel(
    wake_ref, speed_ref, tail_ref, low_ref, high_ref, field_ref, inflow_ref, out_ref,
    all_ref, column_ref, moved_ref, across_ref, lateral_ref, upward_ref,
):
    planes = field_ref.shape[1]
    local_z, local_y = out_ref.shape[1], out_ref.shape[2]
    size = 72
    lane = lax.broadcasted_iota(jnp.int32, (size, 128), 1)
    is_wake = wake_ref[0] != 0
    entering_lane = is_wake & (lane == 0)
    leaving_lane = is_wake & (lane == 127)
    crossing = {o: is_wake & (lane >= 128 - o if o > 0 else lane < -o) for o in (-2, -1, 1, 2)}
    most = fill_speed(speed_ref, tail_ref, low_ref, high_ref, all_ref)
    is_small = TIME_STEP * most < 0.999

    def turned(pair, o):
        first, second = rotated(pair[0], o), rotated(pair[1], o)
        swap = lane < o if o > 0 else lane >= 128 + o
        return jnp.where(swap, second, first), jnp.where(swap, first, second)

    def step(p, small):
        column_ref[...] = jnp.concatenate(
            [inflow_ref[pl.ds(16 * p, 16), :], jnp.zeros((112, 128), F32)], 0
        ).T
        for block in range(72 // size):
            here = slice(size * block, size * block + size)
            kept = slice(8 + size * block, 8 + size * block + size)
            is_end = block == 72 // size - 1

            def velocity(c, plane, t, steps=0):
                row = 8 + size * block + steps
                return all_ref[c, plane, t, row : row + size, :]

            inflow = column_ref[here, :]
            along = []
            for t in range(2):
                along.append(weights(TIME_STEP * velocity(0, p + 1, t), small))
                across = weights(TIME_STEP * velocity(1, p + 1, t), small)
                for o in range(-2, 3):
                    across_ref[o + 2, t, kept, :] = across[o]
                    if is_end:
                        across_ref[o + 2, t, 0:8, :] = across[o][size - 8 :]
            for o in (-2, -1, 1, 2):
                t = 1 if o > 0 else 0
                along[t][o] = jnp.where(crossing[o], 0.0, along[t][o])
            part = [
                [field_ref[c, p, here, 128 * t : 128 * t + 128] for t in range(2)]
                for c in range(3)
            ]
            for c in range(3):
                value = [velocity(c, p + 1, t) for t in range(2)]
                ahead, behind = list(turned(value, -1)), list(turned(value, 1))
                behind[0] = jnp.where(entering_lane, rotated(inflow, -(4 * c + 2)), behind[0])
                ahead[1] = jnp.where(leaving_lane, value[1], ahead[1])
                strength = []
                for t in range(2):
                    strength.append(
                        part[c][t]
                        + (0.5 * TIME_STEP)
                        * (
                            part[0][t] * (ahead[t] - behind[t])
                            + part[1][t] * (velocity(c, p + 1, t, 1) - velocity(c, p + 1, t, -1))
                            + part[2][t] * (velocity(c, p + 2, t) - velocity(c, p, t))
                        )
                    )
                total = [strength[t] * along[t][0] for t in range(2)]
                total[0] = total[0] + jnp.where(lane < 2, rotated(inflow, -4 * c), 0.0)
                for o in (-2, -1, 1, 2):
                    pair = turned([strength[t] * along[t][o] for t in range(2)], o)
                    total = [total[t] + pair[t] for t in range(2)]
                for t in range(2):
                    moved_ref[c, t, kept, :] = total[t]
                    if is_end:
                        moved_ref[c, t, 0:8, :] = total[t][size - 8 :]
        tall = 32
        for block in range(local_y // tall):
            here = slice(tall * block, tall * block + tall)
            for t in range(2):
                total = [jnp.zeros((tall, 128), F32) for _ in range(3)]
                for o in range(-2, 3):
                    first = 8 + tall * block - o
                    weight = across_ref[o + 2, t, first : first + tall, :]
                    for c in range(3):
                        term = moved_ref[c, t, first : first + tall, :] * weight
                        total[c] = term if o == -2 else total[c] + term
                for c in range(3):
                    lateral_ref[c, p, t, here, :] = total[c]
                first = 8 + tall * block
                upward = weights(
                    TIME_STEP * all_ref[2, p + 1, t, first : first + tall, :], small
                )
                for o in range(-2, 3):
                    upward_ref[o + 2, p, t, here, :] = upward[o]

    def run(small):
        def one(p, carry):
            step(p, small)
            return carry

        lax.fori_loop(0, planes, one, 0)

    @pl.when(is_small)
    def _():
        run(True)

    @pl.when(jnp.logical_not(is_small))
    def _():
        run(False)

    def gather(z, carry):
        tall = 32
        for t in range(2):
            for block in range(local_y // tall):
                here = slice(tall * block, tall * block + tall)
                total = [None] * 3
                for o in range(-2, 3):
                    weight = upward_ref[o + 2, z + 2 - o, t, here, :]
                    for c in range(3):
                        term = lateral_ref[c, z + 2 - o, t, here, :] * weight
                        total[c] = term if o == -2 else total[c] + term
                for c in range(3):
                    out_ref[c, z, here, 128 * t : 128 * t + 128] = total[c]
        return carry

    lax.fori_loop(0, local_z, gather, 0)


def call(kernel, shapes, args, smem=(), far=(), scratch=(), limit=24):
    single = not isinstance(shapes, list)
    outs = [jax.ShapeDtypeStruct(s, F32) for s in ([shapes] if single else shapes)]
    def space(i):
        return pltpu.SMEM if i in smem else pltpu.HBM if i in far else pltpu.VMEM

    specs = [pl.BlockSpec(memory_space=space(i)) for i in range(len(args))]
    out = pl.pallas_call(
        kernel,
        out_shape=outs,
        in_specs=specs,
        out_specs=[pl.BlockSpec(memory_space=pltpu.VMEM) for _ in outs],
        scratch_shapes=list(scratch),
        compiler_params=pltpu.CompilerParams(vmem_limit_bytes=limit * 1024 * 1024),
    )(*args)
    return out[0] if single else out


def forward_lines(field):
    count = field.shape[3]
    table = jnp.asarray(forward_table(count))
    scratch = (
        pltpu.VMEM(field.shape, F32),
        pltpu.VMEM(table.shape, BF16),
        pltpu.SemaphoreType.DMA((field.shape[0] + 1,)),
    )
    shape = (count // 2 * 24, 128)
    return call(streamwise_forward, shape, (field, table), far=(0, 1), scratch=scratch, limit=61)


def solve_plane(spectrum, owner, tables):
    count = tables[3].shape[1]
    args = (owner.reshape(1), spectrum, *tables)
    scratch = [pltpu.VMEM((3, 2 * count, count), F32)]
    scratch += [pltpu.VMEM(t.shape, t.dtype) for t in tables]
    scratch += [pltpu.SemaphoreType.DMA((len(tables),))]
    far = (2, 3, 4, 5)
    return call(
        plane_kernel, spectrum.shape, args, smem=(0,), far=far, scratch=scratch, limit=54
    )


def backward_lines(spectrum, drift, table, shape):
    edge = (shape[0] * shape[1] * RIM, shape[3])
    shapes = [shape, shape, edge, edge]
    return call(streamwise_backward, shapes, (spectrum, table, drift), smem=(2,))


def with_edges(speed, above, below):
    comps, local_z, local_y, count = speed.shape
    send = (comps, RIM, local_y + 8, count)
    shapes = [(comps, local_z, 8, count), send, send]
    return call(edge_kernel, shapes, (speed, above, below))


def inflow_columns(wake, speed, tail, low, high, field):
    args = (wake, speed, tail, low, high, field)
    scratch = [pltpu.VMEM((24 * (field.shape[1] + 6), 128), F32)]
    return call(inflow_kernel, (256, 128), args, smem=(0,), scratch=scratch)


def wake_step(wake, speed, tail, low, high, field, inflow):
    comps, local_z, local_y, count = speed.shape
    lanes, planes = count // 128, local_z + 4
    scratch = [
        pltpu.VMEM((comps, planes + 2, lanes, local_y + 24, 128), F32),
        pltpu.VMEM((128, 128), F32),
        pltpu.VMEM((comps, lanes, local_y + 16, 128), F32),
        pltpu.VMEM((5, lanes, local_y + 16, 128), F32),
        pltpu.VMEM((comps, planes, lanes, local_y, 128), F32),
        pltpu.VMEM((5, planes, lanes, local_y, 128), F32),
    ]
    args = (wake, speed, tail, low, high, field, inflow)
    return call(wake_kernel, speed.shape, args, smem=(0,), scratch=scratch)


def from_before(value, axis):
    count = lax.axis_size(axis)
    return lax.ppermute(value, axis, [(i, (i + 1) % count) for i in range(count)])


def from_after(value, axis):
    count = lax.axis_size(axis)
    return lax.ppermute(value, axis, [((i + 1) % count, i) for i in range(count)])


def wider_rows(field):
    above = from_after(field[:, :, :2], "gy")
    below = from_before(field[:, :, field.shape[2] - 2 :], "gy")
    above = jnp.pad(above, ((0, 0), (0, 0), (0, 4), (0, 0)))
    return jnp.concatenate([field, above, below], 2)


def wider_planes(field):
    low = from_before(field[:, field.shape[1] - 2 :], "gz")
    high = from_after(field[:, :2], "gz")
    return jnp.concatenate([low, field, high], 1)


def body(vorticity, wind):
    wake = (lax.axis_index("grp") == 1).astype(jnp.int32).reshape(1)
    field = vorticity[0]
    count_x = field.shape[3]
    size_gz = lax.axis_size("gz")
    groups = lax.axis_size("gy") * size_gz
    owner = lax.axis_index("gy") * size_gz + lax.axis_index("gz")
    axes = ("gy", "gz")
    spectrum = forward_lines(field)
    start = lax.axis_index("grp") * 0
    spectrum, start, halo_field = lax.optimization_barrier((spectrum, start, field))
    spectrum = spectrum.reshape(groups, 24, 128)
    spectrum = lax.all_to_all(spectrum, axes, split_axis=0, concat_axis=0, tiled=True)
    wide = wider_rows(halo_field)
    tables, streamwise = run_time_tables(start, count_x, size_gz)
    spectrum, wide, tables, streamwise = lax.optimization_barrier(
        (spectrum, wide, tables, streamwise)
    )
    spectrum = solve_plane(spectrum, owner, tables)
    spectrum, wide = lax.optimization_barrier((spectrum, wide))
    spectrum = lax.all_to_all(spectrum, axes, split_axis=0, concat_axis=0, tiled=True)
    wide = wider_planes(wide)
    spectrum, wide = lax.optimization_barrier((spectrum, wide))
    spectrum = spectrum.reshape(groups * 24, 128)
    velocity, speed, first, last = backward_lines(spectrum, wind, streamwise, field.shape)
    above, below = from_after(first, "gy"), from_before(last, "gy")
    tail, up, down = with_edges(speed, above, below)
    low, high = from_before(up, "gz"), from_after(down, "gz")
    inflow = inflow_columns(wake, speed, tail, low, high, wide)
    inflow = lax.ppermute(inflow, "grp", [(0, 1)])
    result = wake_step(wake, speed, tail, low, high, wide, inflow)
    return (result[None], velocity[None])


def solution(mesh):
    return jax.shard_map(
        body,
        mesh=mesh,
        in_specs=(P("grp", None, "gz", "gy", None), P("grp", None)),
        out_specs=(P("grp", None, "gz", "gy", None), P("grp", None, "gz", "gy", None)),
        check_vma=False,
    )
```

```python
import math

import jax
import jax.numpy as jnp
import numpy as np
from jax import lax
from jax.experimental import pallas as pl
from jax.experimental.pallas import tpu as pltpu
from jax.sharding import PartitionSpec as P

TIME_STEP = 0.4
RIM = 3
BF16 = jnp.bfloat16
F32 = jnp.float32


def forward_table(count):
    index = np.arange(count)
    phase = (index[:, None] * index[None, :] % count) * (2.0 * math.pi / count)
    half = count // 2
    alternate = 1.0 - 2.0 * (index % 2)
    table = np.concatenate([np.cos(phase[:half]), alternate[None], -np.sin(phase[1:half])], 0)
    table = table.astype(np.float32)
    high = table.astype(BF16)
    return np.stack([high, (table - high.astype(np.float32)).astype(BF16)])


def split(value):
    high = value.astype(BF16)
    low = (value - high.astype(F32)).astype(BF16)
    return high, low


def turns(product, count):
    phase = (product % count).astype(F32) * (2.0 * math.pi / count)
    return jnp.cos(phase), jnp.sin(phase)


def run_time_tables(start, count, blocks):
    def index(shape, dim):
        return lax.broadcasted_iota(jnp.int32, shape, dim) + start

    shape = (2 * count, 2 * count)
    row, col = index(shape, 0), index(shape, 1)
    local = count // blocks

    def place(i):
        return i % count // 8 * local + i % 4 * 2 + i // count

    def part(i):
        return i // 4 % 2

    cosine, sine = turns((row % count) * place(col), count)
    vertical = jnp.where(
        row // count == part(col), cosine, jnp.where(row < count, sine, -sine)
    )
    cosine, sine = turns((col % count) * place(row), count)
    back = jnp.where(
        col // count == part(row), cosine, jnp.where(col < count, sine, -sine)
    ) * (1.0 / (count * count))
    shape = (count, 2 * count)
    cosine, sine = turns(index(shape, 0) * (index(shape, 1) % count), count)
    lateral = jnp.where(index(shape, 1) < count, cosine, sine)
    shape = (count, count)
    row, col = index(shape, 0), index(shape, 1)
    flip = ((row + col) % count == 0).astype(BF16)
    half = count // 2
    cosine, sine = turns((row % half) * col, count)
    alternate = (1 - 2 * (col % 2)).astype(F32)
    scale = jnp.where(row % half == 0, 1.0, 2.0) * (1.0 / count)
    streamwise = jnp.where(
        row < half, cosine * scale, jnp.where(row == half, alternate * scale, -sine * scale)
    )
    def tripled(table, axis):
        high = lax.reduce_precision(table, 8, 7)
        low = (table - high).astype(BF16)
        high = high.astype(BF16)
        return jnp.concatenate([high, high, low], axis)

    plane = (tripled(vertical, 1), tripled(lateral, 0), tripled(back, 1), flip)
    return plane, tripled(streamwise, 0)


def streamwise_forward(field_any, table_any, out_ref, field_ref, table_ref, sems):
    comps, local_z, local_y, count = field_ref.shape
    rows = local_z * local_y
    half = count // 2
    copies = [pltpu.make_async_copy(table_any, table_ref, sems.at[comps])]
    for c in range(comps):
        copies.append(pltpu.make_async_copy(field_any.at[c], field_ref.at[c], sems.at[c]))
    for copy in copies:
        copy.start()
    copies[0].wait()
    dims = (((1,), (1,)), ((), ()))
    for c in range(comps):
        copies[c + 1].wait()
        high, low = split(field_ref[c].reshape(rows, count))

        def term(i, value):
            return lax.dot_general(table_ref[i], value, dims, preferred_element_type=F32)

        result = term(0, high) + term(0, low) + term(1, high)
        for part in range(2):
            for k in range(0, half, 8):
                for a in range(rows // 128):
                    top = part * half + k
                    out_ref[pl.ds(k * 24 + c * 8 + part * 4 + a, 8, stride=24), :] = result[
                        top : top + 8, a * 128 : (a + 1) * 128
                    ]


def product(left, right):
    return jnp.dot(left, right, preferred_element_type=F32)


def left_product(table, value):
    high, low = split(value)
    return product(table, jnp.concatenate([high, low, high], 0))


def right_product(value, table):
    high, low = split(value)
    return product(jnp.concatenate([high, low, high], 1), table)


def signed_waves(index, count, odd):
    signed = jnp.where(index < count // 2, index, index - count)
    if odd:
        signed = jnp.where(index == count // 2, 0, signed)
    return signed.astype(F32) * (2.0 * math.pi / count)


def plane_kernel(
    owner_ref, in_ref, z_any, y_any, back_any, flip_any, out_ref,
    plain_ref, turned_ref, z_ref, y_ref, back_ref, flip_ref, sems,
):
    n = y_ref.shape[1] // 2
    pairs = ((z_any, z_ref), (y_any, y_ref), (back_any, back_ref), (flip_any, flip_ref))
    copies = [pltpu.make_async_copy(s, d, sems.at[i]) for i, (s, d) in enumerate(pairs)]
    for copy in copies:
        copy.start()
    owner = owner_ref[0]
    is_packed = owner == 0
    low_lanes = lax.broadcasted_iota(jnp.int32, (n, 128), 1) < 64
    row = lax.broadcasted_iota(jnp.int32, (n, n), 0)
    col = lax.broadcasted_iota(jnp.int32, (n, n), 1)
    wave_x = owner.astype(F32) * (2.0 * math.pi / n)
    wave_z = signed_waves(row, n, False)
    wave_y = signed_waves(col, n, False)
    curl_z = signed_waves(row, n, True)
    curl_y = signed_waves(col, n, True)
    plane = wave_y * wave_y + wave_z * wave_z
    squared = plane + wave_x * wave_x
    scale = jnp.where(squared > 0, 1.0 / jnp.where(squared > 0, squared, 1.0), 0.0)
    top_scale = 1.0 / (plane + math.pi * math.pi)
    sigma = jnp.where(is_packed, 0.5 * (scale + top_scale), scale)
    delta = 0.5 * (scale - top_scale)
    copies[0].wait()
    copies[1].wait()
    for c in range(3):
        blocks = [
            in_ref[32 * g : 32 * g + 32, 8 * c : 8 * c + 8, :].reshape(n, 128) for g in range(4)
        ]
        tops, bottoms = [], []
        for g in (0, 2):
            first, second = blocks[g], blocks[g + 1]
            tops.append(jnp.where(low_lanes, first, pltpu.roll(second, 64, 1)))
            bottoms.append(jnp.where(low_lanes, pltpu.roll(first, 64, 1), second))
        value = jnp.concatenate(
            [jnp.concatenate(tops, 1), jnp.concatenate(bottoms, 1)], 0
        )
        value = left_product(z_ref[...], value)
        value = right_product(value, y_ref[...])
        real_cos, real_sin = value[:n, :n], value[:n, n:]
        imag_cos, imag_sin = value[n:, :n], value[n:, n:]
        plain_ref[c, :n, :] = (real_cos + imag_sin) * sigma
        plain_ref[c, n:, :] = (imag_cos - real_sin) * sigma
        turned_ref[c, :, :n] = real_cos - imag_sin
        turned_ref[c, :, n:] = imag_cos + real_sin

    copies[3].wait()

    @pl.when(is_packed)
    def _():
        for c in range(3):
            high, low = split(turned_ref[c])
            mirror = product(flip_ref[...], high) + product(flip_ref[...], low)
            plain_ref[c, :n, :] += mirror[:, :n] * delta
            plain_ref[c, n:, :] -= mirror[:, n:] * delta

    copies[2].wait()
    for c in range(3):
        if c == 0:
            def cross(part):
                return curl_y * plain_ref[2, part] - curl_z * plain_ref[1, part]
        elif c == 1:
            def cross(part):
                return curl_z * plain_ref[0, part] - wave_x * plain_ref[2, part]
        else:
            def cross(part):
                return wave_x * plain_ref[1, part] - curl_y * plain_ref[0, part]
        value = jnp.concatenate([-cross(slice(n, 2 * n)), cross(slice(0, n))], 0)
        value = right_product(value, y_ref[...])
        real = value[:n, :n] - value[n:, n:]
        imag = value[n:, :n] + value[:n, n:]
        value = left_product(back_ref[...], jnp.concatenate([real, imag], 0))
        for pair in range(2):
            top = value[:n, 128 * pair : 128 * pair + 128]
            bottom = value[n:, 128 * pair : 128 * pair + 128]
            first = jnp.where(low_lanes, top, pltpu.roll(bottom, 64, 1))
            second = jnp.where(low_lanes, pltpu.roll(top, 64, 1), bottom)
            for g, block in ((2 * pair, first), (2 * pair + 1, second)):
                out_ref[32 * g : 32 * g + 32, 8 * c : 8 * c + 8, :] = block.reshape(32, 8, 128)


def streamwise_backward(
    in_ref, table_ref, drift_ref, out_ref, speed_ref, low_ref, high_ref
):
    comps, local_z, local_y, count = out_ref.shape

    for c in range(comps):
        parts = []
        for part in range(2):
            chunks = [
                in_ref[pl.ds(c * 8 + part * 4 + a, count // 2, stride=24), :] for a in range(4)
            ]
            parts.append(jnp.concatenate(chunks, 1))
        value = jnp.concatenate(parts, 0).T
        result = right_product(value, table_ref[...]) + drift_ref[0, c]
        out_ref[c] = result.reshape(local_z, local_y, count)
        speed_ref[c] = result.reshape(local_z, local_y, count)
    for c in range(comps):
        for z in range(local_z):
            row = (c * local_z + z) * RIM
            low_ref[row : row + RIM, :] = out_ref[c, z, 0:RIM, :]
            high_ref[row : row + RIM, :] = out_ref[c, z, local_y - RIM : local_y, :]


def edge_kernel(speed_ref, above_ref, below_ref, tail_ref, up_ref, down_ref):
    comps, local_z, local_y, count = speed_ref.shape
    for c in range(comps):
        for z in range(local_z):
            row = (c * local_z + z) * RIM
            tail_ref[c, z, 0:RIM, :] = above_ref[row : row + RIM, :]
            tail_ref[c, z, RIM : 8 - RIM, :] = jnp.zeros((8 - 2 * RIM, count), F32)
            tail_ref[c, z, 8 - RIM : 8, :] = below_ref[row : row + RIM, :]
        for target, first in ((up_ref, local_z - RIM), (down_ref, 0)):
            for z in range(RIM):
                target[c, z, 0:local_y, :] = speed_ref[c, first + z]
                target[c, z, local_y : local_y + 8, :] = tail_ref[c, first + z]


def weights(shift, small=False):
    zero = jnp.zeros_like(shift)
    if small:
        left = shift < 0
        frac = jnp.where(left, shift + 1.0, shift)
    else:
        base = jnp.floor(shift)
        frac = shift - base
    rest = 1.0 - frac
    side = -0.5 * frac * rest
    before = side * rest
    after = side * frac
    near = 1.0 + frac * frac * (1.5 * frac - 2.5)
    far = 1.0 - (before + near + after)
    if small:
        values = [zero, before, near, far, after, zero]
        return {o: jnp.where(left, values[o + 3], values[o + 2]) for o in range(-2, 3)}
    at = {k: base == k for k in range(-4, 4)}
    result = {}
    for o in range(-2, 3):
        value = jnp.where(at[o - 2], after, zero)
        value = jnp.where(at[o - 1], far, value)
        value = jnp.where(at[o], near, value)
        result[o] = jnp.where(at[o + 1], before, value)
    return result


def rotated(value, steps):
    return pltpu.roll(value, steps % value.shape[1], 1)


def inflow_kernel(wake_ref, speed_ref, tail_ref, low_ref, high_ref, field_ref, out_ref, line_ref):
    planes, local_z = field_ref.shape[1], speed_ref.shape[1]
    lane = lax.broadcasted_iota(jnp.int32, (72, 128), 1)

    @pl.when(wake_ref[0] == 0)
    def _():
        line_ref[...] = jnp.zeros(line_ref.shape, F32)
        columns = jnp.zeros((72, 128), F32)
        for q in range(planes + 2):
            base = 24 * (q % 5)
            for c in range(3):
                if q < RIM:
                    first, last = low_ref[c, q, :, :128], low_ref[c, q, :, 128:]
                elif q < RIM + local_z:
                    z = q - RIM
                    pieces = [
                        jnp.concatenate([speed_ref[c, z, :, lanes], tail_ref[c, z, :, lanes]], 0)
                        for lanes in (slice(0, 128), slice(128, 256))
                    ]
                    first, last = pieces
                else:
                    z = q - RIM - local_z
                    first, last = high_ref[c, z, :, :128], high_ref[c, z, :, 128:]
                at = base + 4 * c
                here = (lane >= at) & (lane < at + 4)
                ends = jnp.where(lane < 64, first, last)
                columns = jnp.where(here, rotated(ends, at + 3), columns)
                if 1 <= q <= planes:
                    at = base + 12 + 2 * c
                    here = (lane >= at) & (lane < at + 2)
                    columns = jnp.where(
                        here, rotated(field_ref[c, q - 1, :, 128:], at + 2), columns
                    )
            if q % 5 == 4 or q == planes + 1:
                gap = jnp.zeros((40, 128), F32)
                whole = jnp.concatenate([columns, columns[:8], gap, columns[64:]], 0)
                row = 120 * (q // 5)
                line_ref[row : row + 120, :] = whole.T[:120]
                columns = jnp.zeros((72, 128), F32)

        def line(row, plane):
            return line_ref[pl.ds(24 * plane + row, 16, stride=24), :]

        shift = [weights(TIME_STEP * line(x, 1)) for x in (1, 2)]
        part = [[line(12 + 2 * c + x, 1) for x in range(2)] for c in range(3)]
        for c in range(3):
            strength = []
            for x in range(2):
                row = 4 * c + 1 + x
                value = line(row, 1)
                strength.append(
                    part[c][x]
                    + (0.5 * TIME_STEP)
                    * (
                        part[0][x] * (line(row + 1, 1) - line(row - 1, 1))
                        + part[1][x] * (rotated(value, -1) - rotated(value, 1))
                        + part[2][x] * (line(row, 2) - line(row, 0))
                    )
                )
            rows = (
                strength[0] * shift[0][2] + strength[1] * shift[1][1],
                strength[1] * shift[1][2],
                line(4 * c + 2, 1),
            )
            for i, row in enumerate(rows):
                out_ref[pl.ds(4 * c + i, 16, stride=16), :] = row


def fill_speed(speed_ref, tail_ref, low_ref, high_ref, all_ref):
    local_z = speed_ref.shape[1]
    most = jnp.zeros((8, 128), F32)
    for c in range(3):
        for t in range(2):
            lanes = slice(128 * t, 128 * t + 128)
            for own, end, row, first in (
                (low_ref, low_ref, 64, 0),
                (speed_ref, tail_ref, 0, RIM),
                (high_ref, high_ref, 64, RIM + local_z),
            ):
                planes = slice(first, first + own.shape[1])
                body = own[c, :, 0:64, lanes]
                tail = end[c, :, row : row + 8, lanes]
                all_ref[c, planes, t, 8:72, :] = body
                all_ref[c, planes, t, 0:8, :] = tail
                all_ref[c, planes, t, 72:80, :] = tail
                all_ref[c, planes, t, 80:88, :] = body[:, 0:8]
                most = jnp.maximum(most, jnp.max(jnp.abs(body).reshape(-1, 8, 128), 0))
                most = jnp.maximum(most, jnp.max(jnp.abs(tail), 0))
    return jnp.max(most)


def wake_kernel(
    wake_ref, speed_ref, tail_ref, low_ref, high_ref, field_ref, inflow_ref, out_ref,
    all_ref, column_ref, moved_ref, across_ref, lateral_ref, upward_ref,
):
    planes = field_ref.shape[1]
    local_z, local_y = out_ref.shape[1], out_ref.shape[2]
    size = 72
    lane = lax.broadcasted_iota(jnp.int32, (size, 128), 1)
    is_wake = wake_ref[0] != 0
    entering_lane = is_wake & (lane == 0)
    leaving_lane = is_wake & (lane == 127)
    inflow_lanes = is_wake & (lane < 2)
    crossing = {o: is_wake & (lane >= 128 - o if o > 0 else lane < -o) for o in (-2, -1, 1, 2)}
    most = fill_speed(speed_ref, tail_ref, low_ref, high_ref, all_ref)
    for i in range(2):
        column_ref[i] = inflow_ref[128 * i : 128 * i + 128, :].T
    is_small = TIME_STEP * most < 0.999

    def turned(pair, o):
        first, second = rotated(pair[0], o), rotated(pair[1], o)
        swap = lane < o if o > 0 else lane >= 128 + o
        return jnp.where(swap, second, first), jnp.where(swap, first, second)

    def step(p, small):
        for block in range(72 // size):
            here = slice(size * block, size * block + size)
            kept = slice(8 + size * block, 8 + size * block + size)
            is_end = block == 72 // size - 1

            def velocity(c, plane, t, steps=0):
                row = 8 + size * block + steps
                return all_ref[c, plane, t, row : row + size, :]

            inflow = column_ref[p // 8, here, :]
            turn = 128 - 16 * (p % 8)
            along = []
            for t in range(2):
                along.append(weights(TIME_STEP * velocity(0, p + 1, t), small))
                across = weights(TIME_STEP * velocity(1, p + 1, t), small)
                for o in range(-2, 3):
                    across_ref[o + 2, t, kept, :] = across[o]
                    if is_end:
                        across_ref[o + 2, t, 0:8, :] = across[o][size - 8 :]
            for o in (-2, -1, 1, 2):
                t = 1 if o > 0 else 0
                along[t][o] = jnp.where(crossing[o], 0.0, along[t][o])
            part = [
                [field_ref[c, p, here, 128 * t : 128 * t + 128] for t in range(2)]
                for c in range(3)
            ]
            for c in range(3):
                value = [velocity(c, p + 1, t) for t in range(2)]
                ahead, behind = list(turned(value, -1)), list(turned(value, 1))
                entering = pltpu.roll(inflow, turn - (4 * c + 2), 1)
                behind[0] = jnp.where(entering_lane, entering, behind[0])
                ahead[1] = jnp.where(leaving_lane, value[1], ahead[1])
                strength = []
                for t in range(2):
                    strength.append(
                        part[c][t]
                        + (0.5 * TIME_STEP)
                        * (
                            part[0][t] * (ahead[t] - behind[t])
                            + part[1][t] * (velocity(c, p + 1, t, 1) - velocity(c, p + 1, t, -1))
                            + part[2][t] * (velocity(c, p + 2, t) - velocity(c, p, t))
                        )
                    )
                total = [strength[t] * along[t][0] for t in range(2)]
                passed_on = pltpu.roll(inflow, turn - 4 * c, 1)
                total[0] = total[0] + jnp.where(inflow_lanes, passed_on, 0.0)
                for o in (-2, -1, 1, 2):
                    pair = turned([strength[t] * along[t][o] for t in range(2)], o)
                    total = [total[t] + pair[t] for t in range(2)]
                for t in range(2):
                    moved_ref[c, t, kept, :] = total[t]
                    if is_end:
                        moved_ref[c, t, 0:8, :] = total[t][size - 8 :]
        tall = 32
        for block in range(local_y // tall):
            here = slice(tall * block, tall * block + tall)
            for t in range(2):
                total = [jnp.zeros((tall, 128), F32) for _ in range(3)]
                for o in range(-2, 3):
                    first = 8 + tall * block - o
                    weight = across_ref[o + 2, t, first : first + tall, :]
                    for c in range(3):
                        term = moved_ref[c, t, first : first + tall, :] * weight
                        total[c] = term if o == -2 else total[c] + term
                for c in range(3):
                    lateral_ref[c, p, t, here, :] = total[c]
                first = 8 + tall * block
                upward = weights(
                    TIME_STEP * all_ref[2, p + 1, t, first : first + tall, :], small
                )
                for o in range(-2, 3):
                    upward_ref[o + 2, p, t, here, :] = upward[o]

    def run(small):
        def one(p, carry):
            step(p, small)
            return carry

        lax.fori_loop(0, planes, one, 0)

    @pl.when(is_small)
    def _():
        run(True)

    @pl.when(jnp.logical_not(is_small))
    def _():
        run(False)

    def gather(z, carry):
        tall = 32
        for t in range(2):
            for block in range(local_y // tall):
                here = slice(tall * block, tall * block + tall)
                total = [None] * 3
                for o in range(-2, 3):
                    weight = upward_ref[o + 2, z + 2 - o, t, here, :]
                    for c in range(3):
                        term = lateral_ref[c, z + 2 - o, t, here, :] * weight
                        total[c] = term if o == -2 else total[c] + term
                for c in range(3):
                    out_ref[c, z, here, 128 * t : 128 * t + 128] = total[c]
        return carry

    lax.fori_loop(0, local_z, gather, 0)


def call(kernel, shapes, args, smem=(), far=(), scratch=(), limit=24):
    single = not isinstance(shapes, list)
    outs = [jax.ShapeDtypeStruct(s, F32) for s in ([shapes] if single else shapes)]
    def space(i):
        return pltpu.SMEM if i in smem else pltpu.HBM if i in far else pltpu.VMEM

    specs = [pl.BlockSpec(memory_space=space(i)) for i in range(len(args))]
    out = pl.pallas_call(
        kernel,
        out_shape=outs,
        in_specs=specs,
        out_specs=[pl.BlockSpec(memory_space=pltpu.VMEM) for _ in outs],
        scratch_shapes=list(scratch),
        compiler_params=pltpu.CompilerParams(vmem_limit_bytes=limit * 1024 * 1024),
    )(*args)
    return out[0] if single else out


def forward_lines(field):
    count = field.shape[3]
    table = jnp.asarray(forward_table(count))
    scratch = (
        pltpu.VMEM(field.shape, F32),
        pltpu.VMEM(table.shape, BF16),
        pltpu.SemaphoreType.DMA((field.shape[0] + 1,)),
    )
    shape = (count // 2 * 24, 128)
    return call(streamwise_forward, shape, (field, table), far=(0, 1), scratch=scratch, limit=61)


def solve_plane(spectrum, owner, tables):
    count = tables[3].shape[1]
    args = (owner.reshape(1), spectrum, *tables)
    scratch = [pltpu.VMEM((3, 2 * count, count), F32), pltpu.VMEM((3, count, 2 * count), F32)]
    scratch += [pltpu.VMEM(t.shape, t.dtype) for t in tables]
    scratch += [pltpu.SemaphoreType.DMA((len(tables),))]
    far = (2, 3, 4, 5)
    return call(
        plane_kernel, spectrum.shape, args, smem=(0,), far=far, scratch=scratch, limit=54
    )


def backward_lines(spectrum, drift, table, shape):
    edge = (shape[0] * shape[1] * RIM, shape[3])
    shapes = [shape, shape, edge, edge]
    return call(streamwise_backward, shapes, (spectrum, table, drift), smem=(2,))


def with_edges(speed, above, below):
    comps, local_z, local_y, count = speed.shape
    send = (comps, RIM, local_y + 8, count)
    shapes = [(comps, local_z, 8, count), send, send]
    return call(edge_kernel, shapes, (speed, above, below))


def inflow_columns(wake, speed, tail, low, high, field):
    args = (wake, speed, tail, low, high, field)
    scratch = [pltpu.VMEM((24 * (field.shape[1] + 6), 128), F32)]
    return call(inflow_kernel, (256, 128), args, smem=(0,), scratch=scratch)


def wake_step(wake, speed, tail, low, high, field, inflow):
    comps, local_z, local_y, count = speed.shape
    lanes, planes = count // 128, local_z + 4
    scratch = [
        pltpu.VMEM((comps, planes + 2, lanes, local_y + 24, 128), F32),
        pltpu.VMEM((2, 128, 128), F32),
        pltpu.VMEM((comps, lanes, local_y + 16, 128), F32),
        pltpu.VMEM((5, lanes, local_y + 16, 128), F32),
        pltpu.VMEM((comps, planes, lanes, local_y, 128), F32),
        pltpu.VMEM((5, planes, lanes, local_y, 128), F32),
    ]
    args = (wake, speed, tail, low, high, field, inflow)
    return call(wake_kernel, speed.shape, args, smem=(0,), scratch=scratch)


def from_before(value, axis):
    count = lax.axis_size(axis)
    return lax.ppermute(value, axis, [(i, (i + 1) % count) for i in range(count)])


def from_after(value, axis):
    count = lax.axis_size(axis)
    return lax.ppermute(value, axis, [((i + 1) % count, i) for i in range(count)])


def wider_rows(field):
    above = from_after(field[:, :, :2], "gy")
    below = from_before(field[:, :, field.shape[2] - 2 :], "gy")
    above = jnp.pad(above, ((0, 0), (0, 0), (0, 4), (0, 0)))
    return jnp.concatenate([field, above, below], 2)


def wider_planes(field):
    low = from_before(field[:, field.shape[1] - 2 :], "gz")
    high = from_after(field[:, :2], "gz")
    return jnp.concatenate([low, field, high], 1)


def body(vorticity, wind):
    wake = (lax.axis_index("grp") == 1).astype(jnp.int32).reshape(1)
    field = vorticity[0]
    count_x = field.shape[3]
    size_gz = lax.axis_size("gz")
    groups = lax.axis_size("gy") * size_gz
    owner = lax.axis_index("gy") * size_gz + lax.axis_index("gz")
    axes = ("gy", "gz")
    spectrum = forward_lines(field)
    start = lax.axis_index("grp") * 0
    spectrum, start, halo_field, wake = lax.optimization_barrier((spectrum, start, field, wake))
    spectrum = spectrum.reshape(groups, 24, 128)
    spectrum = lax.all_to_all(spectrum, axes, split_axis=0, concat_axis=0, tiled=True)
    wide = wider_rows(halo_field)
    tables, streamwise = run_time_tables(start, count_x, size_gz)
    spectrum, wide, tables, streamwise = lax.optimization_barrier(
        (spectrum, wide, tables, streamwise)
    )
    spectrum = solve_plane(spectrum, owner, tables)
    spectrum, wide = lax.optimization_barrier((spectrum, wide))
    spectrum = lax.all_to_all(spectrum, axes, split_axis=0, concat_axis=0, tiled=True)
    wide = wider_planes(wide)
    spectrum, wide = lax.optimization_barrier((spectrum, wide))
    spectrum = spectrum.reshape(groups * 24, 128)
    velocity, speed, first, last = backward_lines(spectrum, wind, streamwise, field.shape)
    above, below = from_after(first, "gy"), from_before(last, "gy")
    tail, up, down = with_edges(speed, above, below)
    low, high = from_before(up, "gz"), from_after(down, "gz")
    inflow = inflow_columns(wake, speed, tail, low, high, wide)
    inflow = lax.ppermute(inflow, "grp", [(0, 1), (1, 0)])
    result = wake_step(wake, speed, tail, low, high, wide, inflow)
    return (result[None], velocity[None])


def solution(mesh):
    return jax.shard_map(
        body,
        mesh=mesh,
        in_specs=(P("grp", None, "gz", "gy", None), P("grp", None)),
        out_specs=(P("grp", None, "gz", "gy", None), P("grp", None, "gz", "gy", None)),
        check_vma=False,
    )
```

```python
import math

import jax
import jax.numpy as jnp
import numpy as np
from jax import lax
from jax.experimental import pallas as pl
from jax.experimental.pallas import tpu as pltpu
from jax.sharding import PartitionSpec as P

TIME_STEP = 0.4
RIM = 3
BF16 = jnp.bfloat16
F32 = jnp.float32


def forward_table(count):
    index = np.arange(count)
    phase = (index[:, None] * index[None, :] % count) * (2.0 * math.pi / count)
    half = count // 2
    alternate = 1.0 - 2.0 * (index % 2)
    table = np.concatenate([np.cos(phase[:half]), alternate[None], -np.sin(phase[1:half])], 0)
    table = table.astype(np.float32)
    high = table.astype(BF16)
    return np.stack([high, (table - high.astype(np.float32)).astype(BF16)])


def split(value):
    high = value.astype(BF16)
    low = (value - high.astype(F32)).astype(BF16)
    return high, low


def turns(product, count):
    phase = (product % count).astype(F32) * (2.0 * math.pi / count)
    return jnp.cos(phase), jnp.sin(phase)


def run_time_tables(start, count, blocks):
    def index(shape, dim):
        return lax.broadcasted_iota(jnp.int32, shape, dim) + start

    shape = (2 * count, 2 * count)
    row, col = index(shape, 0), index(shape, 1)
    local = count // blocks

    def place(i):
        return i % count // 8 * local + i % 4 * 2 + i // count

    def part(i):
        return i // 4 % 2

    cosine, sine = turns((row % count) * place(col), count)
    vertical = jnp.where(
        row // count == part(col), cosine, jnp.where(row < count, sine, -sine)
    )
    cosine, sine = turns((col % count) * place(row), count)
    back = jnp.where(
        col // count == part(row), cosine, jnp.where(col < count, sine, -sine)
    ) * (1.0 / (count * count))
    shape = (count, 2 * count)
    cosine, sine = turns(index(shape, 0) * (index(shape, 1) % count), count)
    lateral = jnp.where(index(shape, 1) < count, cosine, sine)
    shape = (count, count)
    row, col = index(shape, 0), index(shape, 1)
    flip = ((row + col) % count == 0).astype(BF16)
    half = count // 2
    cosine, sine = turns((row % half) * col, count)
    alternate = (1 - 2 * (col % 2)).astype(F32)
    scale = jnp.where(row % half == 0, 1.0, 2.0) * (1.0 / count)
    streamwise = jnp.where(
        row < half, cosine * scale, jnp.where(row == half, alternate * scale, -sine * scale)
    )
    def tripled(table, axis):
        high = lax.reduce_precision(table, 8, 7)
        low = (table - high).astype(BF16)
        high = high.astype(BF16)
        return jnp.concatenate([high, high, low], axis)

    plane = (tripled(vertical, 1), tripled(lateral, 0), tripled(back, 1), flip)
    return plane, tripled(streamwise, 0)


def streamwise_forward(field_any, table_any, out_ref, field_ref, table_ref, sems):
    comps, local_z, local_y, count = field_ref.shape
    rows = local_z * local_y
    half = count // 2
    copies = [pltpu.make_async_copy(table_any, table_ref, sems.at[comps])]
    for c in range(comps):
        copies.append(pltpu.make_async_copy(field_any.at[c], field_ref.at[c], sems.at[c]))
    for copy in copies:
        copy.start()
    copies[0].wait()
    dims = (((1,), (1,)), ((), ()))
    for c in range(comps):
        copies[c + 1].wait()
        high, low = split(field_ref[c].reshape(rows, count))

        def term(i, value):
            return lax.dot_general(table_ref[i], value, dims, preferred_element_type=F32)

        result = term(0, high) + term(0, low) + term(1, high)
        for part in range(2):
            for k in range(0, half, 8):
                for a in range(rows // 128):
                    top = part * half + k
                    out_ref[pl.ds(k * 24 + c * 8 + part * 4 + a, 8, stride=24), :] = result[
                        top : top + 8, a * 128 : (a + 1) * 128
                    ]


def product(left, right):
    return jnp.dot(left, right, preferred_element_type=F32)


def left_product(table, value):
    high, low = split(value)
    return product(table, jnp.concatenate([high, low, high], 0))


def right_product(value, table):
    high, low = split(value)
    return product(jnp.concatenate([high, low, high], 1), table)


def signed_waves(index, count, odd):
    signed = jnp.where(index < count // 2, index, index - count)
    if odd:
        signed = jnp.where(index == count // 2, 0, signed)
    return signed.astype(F32) * (2.0 * math.pi / count)


def plane_kernel(
    owner_ref, in_any, z_any, y_any, back_any, flip_any, out_ref,
    in_ref, plain_ref, turned_ref, z_ref, y_ref, back_ref, flip_ref, sems,
):
    n = y_ref.shape[1] // 2
    pairs = (
        (z_any, z_ref), (y_any, y_ref), (back_any, back_ref), (flip_any, flip_ref), (in_any, in_ref)
    )
    copies = [pltpu.make_async_copy(s, d, sems.at[i]) for i, (s, d) in enumerate(pairs)]
    for i in (0, 4, 1, 2, 3):
        copies[i].start()
    owner = owner_ref[0]
    is_packed = owner == 0
    low_lanes = lax.broadcasted_iota(jnp.int32, (n, 128), 1) < 64
    row = lax.broadcasted_iota(jnp.int32, (n, n), 0)
    col = lax.broadcasted_iota(jnp.int32, (n, n), 1)
    wave_x = owner.astype(F32) * (2.0 * math.pi / n)
    wave_z = signed_waves(row, n, False)
    wave_y = signed_waves(col, n, False)
    curl_z = signed_waves(row, n, True)
    curl_y = signed_waves(col, n, True)
    plane = wave_y * wave_y + wave_z * wave_z
    squared = plane + wave_x * wave_x
    scale = jnp.where(squared > 0, 1.0 / jnp.where(squared > 0, squared, 1.0), 0.0)
    top_scale = 1.0 / (plane + math.pi * math.pi)
    sigma = jnp.where(is_packed, 0.5 * (scale + top_scale), scale)
    delta = 0.5 * (scale - top_scale)
    copies[0].wait()
    copies[4].wait()
    copies[1].wait()
    for c in range(3):
        blocks = [
            in_ref[32 * g : 32 * g + 32, 8 * c : 8 * c + 8, :].reshape(n, 128) for g in range(4)
        ]
        tops, bottoms = [], []
        for g in (0, 2):
            first, second = blocks[g], blocks[g + 1]
            tops.append(jnp.where(low_lanes, first, pltpu.roll(second, 64, 1)))
            bottoms.append(jnp.where(low_lanes, pltpu.roll(first, 64, 1), second))
        value = jnp.concatenate(
            [jnp.concatenate(tops, 1), jnp.concatenate(bottoms, 1)], 0
        )
        value = left_product(z_ref[...], value)
        value = right_product(value, y_ref[...])
        real_cos, real_sin = value[:n, :n], value[:n, n:]
        imag_cos, imag_sin = value[n:, :n], value[n:, n:]
        plain_ref[c, :n, :] = (real_cos + imag_sin) * sigma
        plain_ref[c, n:, :] = (imag_cos - real_sin) * sigma
        turned_ref[c, :, :n] = real_cos - imag_sin
        turned_ref[c, :, n:] = imag_cos + real_sin

    copies[3].wait()

    @pl.when(is_packed)
    def _():
        for c in range(3):
            high, low = split(turned_ref[c])
            mirror = product(flip_ref[...], high) + product(flip_ref[...], low)
            plain_ref[c, :n, :] += mirror[:, :n] * delta
            plain_ref[c, n:, :] -= mirror[:, n:] * delta

    copies[2].wait()
    for c in range(3):
        if c == 0:
            def cross(part):
                return curl_y * plain_ref[2, part] - curl_z * plain_ref[1, part]
        elif c == 1:
            def cross(part):
                return curl_z * plain_ref[0, part] - wave_x * plain_ref[2, part]
        else:
            def cross(part):
                return wave_x * plain_ref[1, part] - curl_y * plain_ref[0, part]
        value = jnp.concatenate([-cross(slice(n, 2 * n)), cross(slice(0, n))], 0)
        value = right_product(value, y_ref[...])
        real = value[:n, :n] - value[n:, n:]
        imag = value[n:, :n] + value[:n, n:]
        value = left_product(back_ref[...], jnp.concatenate([real, imag], 0))
        for pair in range(2):
            top = value[:n, 128 * pair : 128 * pair + 128]
            bottom = value[n:, 128 * pair : 128 * pair + 128]
            first = jnp.where(low_lanes, top, pltpu.roll(bottom, 64, 1))
            second = jnp.where(low_lanes, pltpu.roll(top, 64, 1), bottom)
            for g, block in ((2 * pair, first), (2 * pair + 1, second)):
                out_ref[32 * g : 32 * g + 32, 8 * c : 8 * c + 8, :] = block.reshape(32, 8, 128)


def streamwise_backward(
    in_ref, table_ref, drift_ref, out_ref, low_ref, high_ref
):
    comps, local_z, local_y, count = out_ref.shape

    for c in range(comps):
        parts = []
        for part in range(2):
            chunks = [
                in_ref[pl.ds(c * 8 + part * 4 + a, count // 2, stride=24), :] for a in range(4)
            ]
            parts.append(jnp.concatenate(chunks, 1))
        value = jnp.concatenate(parts, 0).T
        result = right_product(value, table_ref[...]) + drift_ref[0, c]
        out_ref[c] = result.reshape(local_z, local_y, count)
    for c in range(comps):
        for z in range(local_z):
            row = (c * local_z + z) * RIM
            low_ref[row : row + RIM, :] = out_ref[c, z, 0:RIM, :]
            high_ref[row : row + RIM, :] = out_ref[c, z, local_y - RIM : local_y, :]


def edge_kernel(speed_ref, above_ref, below_ref, tail_ref, up_ref, down_ref):
    comps, local_z, local_y, count = speed_ref.shape
    for c in range(comps):
        for z in range(local_z):
            row = (c * local_z + z) * RIM
            tail_ref[c, z, 0:RIM, :] = above_ref[row : row + RIM, :]
            tail_ref[c, z, RIM : 8 - RIM, :] = jnp.zeros((8 - 2 * RIM, count), F32)
            tail_ref[c, z, 8 - RIM : 8, :] = below_ref[row : row + RIM, :]
        for target, first in ((up_ref, local_z - RIM), (down_ref, 0)):
            for z in range(RIM):
                target[c, z, 0:local_y, :] = speed_ref[c, first + z]
                target[c, z, local_y : local_y + 8, :] = tail_ref[c, first + z]


def weights(shift, small=False):
    zero = jnp.zeros_like(shift)
    if small:
        left = shift < 0
        frac = jnp.where(left, shift + 1.0, shift)
    else:
        base = jnp.floor(shift)
        frac = shift - base
    rest = 1.0 - frac
    side = -0.5 * frac * rest
    before = side * rest
    after = side * frac
    near = 1.0 + frac * frac * (1.5 * frac - 2.5)
    far = 1.0 - (before + near + after)
    if small:
        values = [zero, before, near, far, after, zero]
        return {o: jnp.where(left, values[o + 3], values[o + 2]) for o in range(-2, 3)}
    at = {k: base == k for k in range(-4, 4)}
    result = {}
    for o in range(-2, 3):
        value = jnp.where(at[o - 2], after, zero)
        value = jnp.where(at[o - 1], far, value)
        value = jnp.where(at[o], near, value)
        result[o] = jnp.where(at[o + 1], before, value)
    return result


def rotated(value, steps):
    return pltpu.roll(value, steps % value.shape[1], 1)


def inflow_kernel(wake_ref, speed_ref, tail_ref, low_ref, high_ref, field_ref, out_ref, line_ref):
    planes, local_z = field_ref.shape[1], speed_ref.shape[1]
    lane = lax.broadcasted_iota(jnp.int32, (72, 128), 1)

    @pl.when(wake_ref[0] == 0)
    def _():
        line_ref[...] = jnp.zeros(line_ref.shape, F32)
        columns = jnp.zeros((72, 128), F32)
        for q in range(planes + 2):
            base = 24 * (q % 5)
            for c in range(3):
                if q < RIM:
                    first, last = low_ref[c, q, :, :128], low_ref[c, q, :, 128:]
                elif q < RIM + local_z:
                    z = q - RIM
                    pieces = [
                        jnp.concatenate([speed_ref[c, z, :, lanes], tail_ref[c, z, :, lanes]], 0)
                        for lanes in (slice(0, 128), slice(128, 256))
                    ]
                    first, last = pieces
                else:
                    z = q - RIM - local_z
                    first, last = high_ref[c, z, :, :128], high_ref[c, z, :, 128:]
                at = base + 4 * c
                here = (lane >= at) & (lane < at + 4)
                ends = jnp.where(lane < 64, first, last)
                columns = jnp.where(here, rotated(ends, at + 3), columns)
                if 1 <= q <= planes:
                    at = base + 12 + 2 * c
                    here = (lane >= at) & (lane < at + 2)
                    columns = jnp.where(
                        here, rotated(field_ref[c, q - 1, :, 128:], at + 2), columns
                    )
            if q % 5 == 4 or q == planes + 1:
                gap = jnp.zeros((40, 128), F32)
                whole = jnp.concatenate([columns, columns[:8], gap, columns[64:]], 0)
                row = 120 * (q // 5)
                line_ref[row : row + 120, :] = whole.T[:120]
                columns = jnp.zeros((72, 128), F32)

        def line(row, plane):
            return line_ref[pl.ds(24 * plane + row, 16, stride=24), :]

        shift = [weights(TIME_STEP * line(x, 1)) for x in (1, 2)]
        part = [[line(12 + 2 * c + x, 1) for x in range(2)] for c in range(3)]
        for c in range(3):
            strength = []
            for x in range(2):
                row = 4 * c + 1 + x
                value = line(row, 1)
                strength.append(
                    part[c][x]
                    + (0.5 * TIME_STEP)
                    * (
                        part[0][x] * (line(row + 1, 1) - line(row - 1, 1))
                        + part[1][x] * (rotated(value, -1) - rotated(value, 1))
                        + part[2][x] * (line(row, 2) - line(row, 0))
                    )
                )
            rows = (
                strength[0] * shift[0][2] + strength[1] * shift[1][1],
                strength[1] * shift[1][2],
                line(4 * c + 2, 1),
            )
            for i in range(2):
                out_ref[pl.ds(2 * planes * c + i, planes, stride=2), :] = rows[i][:planes]
            first = 6 * planes + planes * c
            out_ref[first : first + planes, :] = rows[2][:planes]


def fill_speed(speed_ref, tail_ref, low_ref, high_ref, all_ref):
    local_z = speed_ref.shape[1]
    most = jnp.zeros((8, 128), F32)
    for c in range(3):
        for t in range(2):
            lanes = slice(128 * t, 128 * t + 128)
            for own, end, row, first in (
                (low_ref, low_ref, 64, 0),
                (speed_ref, tail_ref, 0, RIM),
                (high_ref, high_ref, 64, RIM + local_z),
            ):
                planes = slice(first, first + own.shape[1])
                body = own[c, :, 0:64, lanes]
                tail = end[c, :, row : row + 8, lanes]
                all_ref[c, planes, t, 8:72, :] = body
                all_ref[c, planes, t, 0:8, :] = tail
                all_ref[c, planes, t, 72:80, :] = tail
                all_ref[c, planes, t, 80:88, :] = body[:, 0:8]
                most = jnp.maximum(most, jnp.max(jnp.abs(body).reshape(-1, 8, 128), 0))
                most = jnp.maximum(most, jnp.max(jnp.abs(tail), 0))
    return jnp.max(most)


def wake_kernel(
    wake_ref, speed_ref, tail_ref, low_ref, high_ref, field_ref, inflow_ref, out_ref, speed_any,
    all_ref, column_ref, moved_ref, across_ref, lateral_ref, upward_ref, sem,
):
    copy = pltpu.make_async_copy(speed_ref, speed_any, sem)
    copy.start()
    planes = field_ref.shape[1]
    local_z, local_y = out_ref.shape[1], out_ref.shape[2]
    size = 72
    lane = lax.broadcasted_iota(jnp.int32, (size, 128), 1)
    is_wake = wake_ref[0] != 0
    entering_lane = is_wake & (lane == 0)
    leaving_lane = is_wake & (lane == 127)
    inflow_lanes = is_wake & (lane < 2)
    crossing = {o: is_wake & (lane >= 128 - o if o > 0 else lane < -o) for o in (-2, -1, 1, 2)}
    most = fill_speed(speed_ref, tail_ref, low_ref, high_ref, all_ref)
    missing = 128 - inflow_ref.shape[0]
    column_ref[...] = jnp.concatenate([inflow_ref[...], jnp.zeros((missing, 128), F32)], 0).T
    is_small = TIME_STEP * most < 0.999

    def turned(pair, o):
        first, second = rotated(pair[0], o), rotated(pair[1], o)
        swap = lane < o if o > 0 else lane >= 128 + o
        return jnp.where(swap, second, first), jnp.where(swap, first, second)

    def step(p, small):
        for block in range(72 // size):
            here = slice(size * block, size * block + size)
            kept = slice(8 + size * block, 8 + size * block + size)
            is_end = block == 72 // size - 1

            def velocity(c, plane, t, steps=0):
                row = 8 + size * block + steps
                return all_ref[c, plane, t, row : row + size, :]

            inflow = column_ref[here, :]
            along = []
            for t in range(2):
                along.append(weights(TIME_STEP * velocity(0, p + 1, t), small))
                across = weights(TIME_STEP * velocity(1, p + 1, t), small)
                for o in range(-2, 3):
                    across_ref[o + 2, t, kept, :] = across[o]
                    if is_end:
                        across_ref[o + 2, t, 0:8, :] = across[o][size - 8 :]
            for o in (-2, -1, 1, 2):
                t = 1 if o > 0 else 0
                along[t][o] = jnp.where(crossing[o], 0.0, along[t][o])
            part = [
                [field_ref[c, p, here, 128 * t : 128 * t + 128] for t in range(2)]
                for c in range(3)
            ]
            for c in range(3):
                value = [velocity(c, p + 1, t) for t in range(2)]
                ahead, behind = list(turned(value, -1)), list(turned(value, 1))
                entering = pltpu.roll(inflow, 128 - (6 + c) * planes - p, 1)
                behind[0] = jnp.where(entering_lane, entering, behind[0])
                ahead[1] = jnp.where(leaving_lane, value[1], ahead[1])
                strength = []
                for t in range(2):
                    strength.append(
                        part[c][t]
                        + (0.5 * TIME_STEP)
                        * (
                            part[0][t] * (ahead[t] - behind[t])
                            + part[1][t] * (velocity(c, p + 1, t, 1) - velocity(c, p + 1, t, -1))
                            + part[2][t] * (velocity(c, p + 2, t) - velocity(c, p, t))
                        )
                    )
                total = [strength[t] * along[t][0] for t in range(2)]
                passed_on = pltpu.roll(inflow, 128 - 2 * planes * c - 2 * p, 1)
                total[0] = total[0] + jnp.where(inflow_lanes, passed_on, 0.0)
                for o in (-2, -1, 1, 2):
                    pair = turned([strength[t] * along[t][o] for t in range(2)], o)
                    total = [total[t] + pair[t] for t in range(2)]
                for t in range(2):
                    moved_ref[c, t, kept, :] = total[t]
                    if is_end:
                        moved_ref[c, t, 0:8, :] = total[t][size - 8 :]
        tall = 32
        for block in range(local_y // tall):
            here = slice(tall * block, tall * block + tall)
            for t in range(2):
                total = [jnp.zeros((tall, 128), F32) for _ in range(3)]
                for o in range(-2, 3):
                    first = 8 + tall * block - o
                    weight = across_ref[o + 2, t, first : first + tall, :]
                    for c in range(3):
                        term = moved_ref[c, t, first : first + tall, :] * weight
                        total[c] = term if o == -2 else total[c] + term
                for c in range(3):
                    lateral_ref[c, p, t, here, :] = total[c]
                first = 8 + tall * block
                upward = weights(
                    TIME_STEP * all_ref[2, p + 1, t, first : first + tall, :], small
                )
                for o in range(-2, 3):
                    upward_ref[o + 2, p, t, here, :] = upward[o]

    def run(small):
        def one(p, carry):
            step(p, small)
            return carry

        lax.fori_loop(0, planes, one, 0)

    @pl.when(is_small)
    def _():
        run(True)

    @pl.when(jnp.logical_not(is_small))
    def _():
        run(False)

    def gather(z, carry):
        tall = 32
        for t in range(2):
            for block in range(local_y // tall):
                here = slice(tall * block, tall * block + tall)
                total = [None] * 3
                for o in range(-2, 3):
                    weight = upward_ref[o + 2, z + 2 - o, t, here, :]
                    for c in range(3):
                        term = lateral_ref[c, z + 2 - o, t, here, :] * weight
                        total[c] = term if o == -2 else total[c] + term
                for c in range(3):
                    out_ref[c, z, here, 128 * t : 128 * t + 128] = total[c]
        return carry

    lax.fori_loop(0, local_z, gather, 0)
    copy.wait()


def call(kernel, shapes, args, smem=(), far=(), far_out=(), scratch=(), limit=24):
    single = not isinstance(shapes, list)
    outs = [jax.ShapeDtypeStruct(s, F32) for s in ([shapes] if single else shapes)]
    def space(i):
        return pltpu.SMEM if i in smem else pltpu.HBM if i in far else pltpu.VMEM

    specs = [pl.BlockSpec(memory_space=space(i)) for i in range(len(args))]
    out = pl.pallas_call(
        kernel,
        out_shape=outs,
        in_specs=specs,
        out_specs=[
            pl.BlockSpec(memory_space=pltpu.HBM if i in far_out else pltpu.VMEM)
            for i in range(len(outs))
        ],
        scratch_shapes=list(scratch),
        compiler_params=pltpu.CompilerParams(vmem_limit_bytes=limit * 1024 * 1024),
    )(*args)
    return out[0] if single else out


def forward_lines(field):
    count = field.shape[3]
    table = jnp.asarray(forward_table(count))
    scratch = (
        pltpu.VMEM(field.shape, F32),
        pltpu.VMEM(table.shape, BF16),
        pltpu.SemaphoreType.DMA((field.shape[0] + 1,)),
    )
    shape = (count // 2 * 24, 128)
    return call(streamwise_forward, shape, (field, table), far=(0, 1), scratch=scratch, limit=61)


def solve_plane(spectrum, owner, tables):
    count = tables[3].shape[1]
    args = (owner.reshape(1), spectrum, *tables)
    scratch = [pltpu.VMEM(spectrum.shape, F32)]
    scratch += [pltpu.VMEM((3, 2 * count, count), F32), pltpu.VMEM((3, count, 2 * count), F32)]
    scratch += [pltpu.VMEM(t.shape, t.dtype) for t in tables]
    scratch += [pltpu.SemaphoreType.DMA((len(tables) + 1,))]
    far = (1, 2, 3, 4, 5)
    return call(
        plane_kernel, spectrum.shape, args, smem=(0,), far=far, scratch=scratch, limit=54
    )


def backward_lines(spectrum, drift, table, shape):
    edge = (shape[0] * shape[1] * RIM, shape[3])
    shapes = [shape, edge, edge]
    return call(streamwise_backward, shapes, (spectrum, table, drift), smem=(2,))


def with_edges(speed, above, below):
    comps, local_z, local_y, count = speed.shape
    send = (comps, RIM, local_y + 8, count)
    shapes = [(comps, local_z, 8, count), send, send]
    return call(edge_kernel, shapes, (speed, above, below))


def inflow_columns(wake, speed, tail, low, high, field):
    args = (wake, speed, tail, low, high, field)
    scratch = [pltpu.VMEM((24 * (field.shape[1] + 6), 128), F32)]
    shape = (9 * field.shape[1] + 4, 128)
    return call(inflow_kernel, shape, args, smem=(0,), scratch=scratch)


def wake_step(wake, speed, tail, low, high, field, inflow):
    comps, local_z, local_y, count = speed.shape
    lanes, planes = count // 128, local_z + 4
    scratch = [
        pltpu.VMEM((comps, planes + 2, lanes, local_y + 24, 128), F32),
        pltpu.VMEM((128, 128), F32),
        pltpu.VMEM((comps, lanes, local_y + 16, 128), F32),
        pltpu.VMEM((5, lanes, local_y + 16, 128), F32),
        pltpu.VMEM((comps, planes, lanes, local_y, 128), F32),
        pltpu.VMEM((5, planes, lanes, local_y, 128), F32),
        pltpu.SemaphoreType.DMA,
    ]
    args = (wake, speed, tail, low, high, field, inflow)
    shapes = [speed.shape, speed.shape]
    return call(wake_kernel, shapes, args, smem=(0,), far_out=(1,), scratch=scratch)


def from_before(value, axis):
    count = lax.axis_size(axis)
    return lax.ppermute(value, axis, [(i, (i + 1) % count) for i in range(count)])


def from_after(value, axis):
    count = lax.axis_size(axis)
    return lax.ppermute(value, axis, [((i + 1) % count, i) for i in range(count)])


def wider_rows(field):
    above = from_after(field[:, :, :2], "gy")
    below = from_before(field[:, :, field.shape[2] - 2 :], "gy")
    above = jnp.pad(above, ((0, 0), (0, 0), (0, 4), (0, 0)))
    return jnp.concatenate([field, above, below], 2)


def wider_planes(field):
    low = from_before(field[:, field.shape[1] - 2 :], "gz")
    high = from_after(field[:, :2], "gz")
    return jnp.concatenate([low, field, high], 1)


def body(vorticity, wind):
    wake = (lax.axis_index("grp") == 1).astype(jnp.int32).reshape(1)
    field = vorticity[0]
    count_x = field.shape[3]
    size_gz = lax.axis_size("gz")
    groups = lax.axis_size("gy") * size_gz
    owner = lax.axis_index("gy") * size_gz + lax.axis_index("gz")
    axes = ("gy", "gz")
    spectrum = forward_lines(field)
    start = lax.axis_index("grp") * 0
    spectrum, start, halo_field, wake = lax.optimization_barrier((spectrum, start, field, wake))
    spectrum = spectrum.reshape(groups, 24, 128)
    spectrum = lax.all_to_all(spectrum, axes, split_axis=0, concat_axis=0, tiled=True)
    wide = wider_rows(halo_field)
    tables, streamwise = run_time_tables(start, count_x, size_gz)
    spectrum, wide, tables, streamwise = lax.optimization_barrier(
        (spectrum, wide, tables, streamwise)
    )
    spectrum = solve_plane(spectrum, owner, tables)
    spectrum, wide = lax.optimization_barrier((spectrum, wide))
    spectrum = lax.all_to_all(spectrum, axes, split_axis=0, concat_axis=0, tiled=True)
    wide = wider_planes(wide)
    spectrum, wide = lax.optimization_barrier((spectrum, wide))
    spectrum = spectrum.reshape(groups * 24, 128)
    speed, first, last = backward_lines(spectrum, wind, streamwise, field.shape)
    above, below = from_after(first, "gy"), from_before(last, "gy")
    tail, up, down = with_edges(speed, above, below)
    low, high = from_before(up, "gz"), from_after(down, "gz")
    inflow = inflow_columns(wake, speed, tail, low, high, wide)
    inflow = lax.ppermute(inflow, "grp", [(0, 1)])
    result, velocity = wake_step(wake, speed, tail, low, high, wide, inflow)
    return (result[None], velocity[None])


def solution(mesh):
    return jax.shard_map(
        body,
        mesh=mesh,
        in_specs=(P("grp", None, "gz", "gy", None), P("grp", None)),
        out_specs=(P("grp", None, "gz", "gy", None), P("grp", None, "gz", "gy", None)),
        check_vma=False,
    )
```

```python
import math

import jax
import jax.numpy as jnp
import numpy as np
from jax import lax
from jax.experimental import pallas as pl
from jax.experimental.pallas import tpu as pltpu
from jax.sharding import PartitionSpec as P

TIME_STEP = 0.4
RIM = 3
BF16 = jnp.bfloat16
F32 = jnp.float32


def forward_table(count):
    index = np.arange(count)
    phase = (index[:, None] * index[None, :] % count) * (2.0 * math.pi / count)
    half = count // 2
    alternate = 1.0 - 2.0 * (index % 2)
    table = np.concatenate([np.cos(phase[:half]), alternate[None], -np.sin(phase[1:half])], 0)
    table = table.astype(np.float32)
    high = table.astype(BF16)
    return np.stack([high, (table - high.astype(np.float32)).astype(BF16)])


def split(value):
    high = value.astype(BF16)
    low = (value - high.astype(F32)).astype(BF16)
    return high, low


def turns(product, count):
    phase = (product % count).astype(F32) * (2.0 * math.pi / count)
    return jnp.cos(phase), jnp.sin(phase)


def run_time_tables(start, count, blocks):
    def index(shape, dim):
        return lax.broadcasted_iota(jnp.int32, shape, dim) + start

    shape = (2 * count, 2 * count)
    row, col = index(shape, 0), index(shape, 1)
    local = count // blocks

    def place(i):
        return i % count // 8 * local + i % 4 * 2 + i // count

    def part(i):
        return i // 4 % 2

    cosine, sine = turns((row % count) * place(col), count)
    vertical = jnp.where(
        row // count == part(col), cosine, jnp.where(row < count, sine, -sine)
    )
    cosine, sine = turns((col % count) * place(row), count)
    back = jnp.where(
        col // count == part(row), cosine, jnp.where(col < count, sine, -sine)
    ) * (1.0 / (count * count))
    shape = (count, 2 * count)
    cosine, sine = turns(index(shape, 0) * (index(shape, 1) % count), count)
    lateral = jnp.where(index(shape, 1) < count, cosine, sine)
    shape = (count, count)
    row, col = index(shape, 0), index(shape, 1)
    flip = ((row + col) % count == 0).astype(BF16)
    half = count // 2
    cosine, sine = turns((row % half) * col, count)
    alternate = (1 - 2 * (col % 2)).astype(F32)
    scale = jnp.where(row % half == 0, 1.0, 2.0) * (1.0 / count)
    streamwise = jnp.where(
        row < half, cosine * scale, jnp.where(row == half, alternate * scale, -sine * scale)
    )
    def tripled(table, axis):
        high = lax.reduce_precision(table, 8, 7)
        low = (table - high).astype(BF16)
        high = high.astype(BF16)
        return jnp.concatenate([high, high, low], axis)

    plane = (tripled(vertical, 1), tripled(lateral, 0), tripled(back, 1), flip)
    return plane, tripled(streamwise, 0)


def streamwise_forward(field_any, table_any, out_ref, field_ref, table_ref, sems):
    comps, local_z, local_y, count = field_ref.shape
    rows = local_z * local_y
    half = count // 2
    copies = [pltpu.make_async_copy(table_any, table_ref, sems.at[comps])]
    for c in range(comps):
        copies.append(pltpu.make_async_copy(field_any.at[c], field_ref.at[c], sems.at[c]))
    for copy in copies:
        copy.start()
    copies[0].wait()
    dims = (((1,), (1,)), ((), ()))
    for c in range(comps):
        copies[c + 1].wait()
        high, low = split(field_ref[c].reshape(rows, count))

        def term(i, value):
            return lax.dot_general(table_ref[i], value, dims, preferred_element_type=F32)

        result = term(0, high) + term(0, low) + term(1, high)
        for part in range(2):
            for k in range(0, half, 8):
                for a in range(rows // 128):
                    top = part * half + k
                    out_ref[pl.ds(k * 24 + c * 8 + part * 4 + a, 8, stride=24), :] = result[
                        top : top + 8, a * 128 : (a + 1) * 128
                    ]


def product(left, right):
    return jnp.dot(left, right, preferred_element_type=F32)


def left_product(table, value):
    high, low = split(value)
    return product(table, jnp.concatenate([high, low, high], 0))


def right_product(value, table):
    high, low = split(value)
    return product(jnp.concatenate([high, low, high], 1), table)


def signed_waves(index, count, odd):
    signed = jnp.where(index < count // 2, index, index - count)
    if odd:
        signed = jnp.where(index == count // 2, 0, signed)
    return signed.astype(F32) * (2.0 * math.pi / count)


def plane_kernel(
    owner_ref, in_any, z_any, y_any, back_any, flip_any, out_ref,
    in_ref, plain_ref, turned_ref, z_ref, y_ref, back_ref, flip_ref, sems,
):
    n = y_ref.shape[1] // 2
    pairs = (
        (z_any, z_ref), (y_any, y_ref), (back_any, back_ref), (flip_any, flip_ref), (in_any, in_ref)
    )
    copies = [pltpu.make_async_copy(s, d, sems.at[i]) for i, (s, d) in enumerate(pairs)]
    for i in (0, 4, 1, 2, 3):
        copies[i].start()
    owner = owner_ref[0]
    is_packed = owner == 0
    low_lanes = lax.broadcasted_iota(jnp.int32, (n, 128), 1) < 64
    row = lax.broadcasted_iota(jnp.int32, (n, n), 0)
    col = lax.broadcasted_iota(jnp.int32, (n, n), 1)
    wave_x = owner.astype(F32) * (2.0 * math.pi / n)
    wave_z = signed_waves(row, n, False)
    wave_y = signed_waves(col, n, False)
    curl_z = signed_waves(row, n, True)
    curl_y = signed_waves(col, n, True)
    plane = wave_y * wave_y + wave_z * wave_z
    squared = plane + wave_x * wave_x
    scale = jnp.where(squared > 0, 1.0 / jnp.where(squared > 0, squared, 1.0), 0.0)
    top_scale = 1.0 / (plane + math.pi * math.pi)
    sigma = jnp.where(is_packed, 0.5 * (scale + top_scale), scale)
    delta = 0.5 * (scale - top_scale)
    copies[0].wait()
    copies[4].wait()
    copies[1].wait()
    for c in range(3):
        blocks = [
            in_ref[32 * g : 32 * g + 32, 8 * c : 8 * c + 8, :].reshape(n, 128) for g in range(4)
        ]
        tops, bottoms = [], []
        for g in (0, 2):
            first, second = blocks[g], blocks[g + 1]
            tops.append(jnp.where(low_lanes, first, pltpu.roll(second, 64, 1)))
            bottoms.append(jnp.where(low_lanes, pltpu.roll(first, 64, 1), second))
        value = jnp.concatenate(
            [jnp.concatenate(tops, 1), jnp.concatenate(bottoms, 1)], 0
        )
        value = left_product(z_ref[...], value)
        value = right_product(value, y_ref[...])
        real_cos, real_sin = value[:n, :n], value[:n, n:]
        imag_cos, imag_sin = value[n:, :n], value[n:, n:]
        plain_ref[c, :n, :] = (real_cos + imag_sin) * sigma
        plain_ref[c, n:, :] = (imag_cos - real_sin) * sigma
        turned_ref[c, :, :n] = real_cos - imag_sin
        turned_ref[c, :, n:] = imag_cos + real_sin

    copies[3].wait()

    @pl.when(is_packed)
    def _():
        for c in range(3):
            high, low = split(turned_ref[c])
            mirror = product(flip_ref[...], high) + product(flip_ref[...], low)
            plain_ref[c, :n, :] += mirror[:, :n] * delta
            plain_ref[c, n:, :] -= mirror[:, n:] * delta

    copies[2].wait()
    for c in range(3):
        if c == 0:
            def cross(part):
                return curl_y * plain_ref[2, part] - curl_z * plain_ref[1, part]
        elif c == 1:
            def cross(part):
                return curl_z * plain_ref[0, part] - wave_x * plain_ref[2, part]
        else:
            def cross(part):
                return wave_x * plain_ref[1, part] - curl_y * plain_ref[0, part]
        value = jnp.concatenate([-cross(slice(n, 2 * n)), cross(slice(0, n))], 0)
        value = right_product(value, y_ref[...])
        real = value[:n, :n] - value[n:, n:]
        imag = value[n:, :n] + value[:n, n:]
        value = left_product(back_ref[...], jnp.concatenate([real, imag], 0))
        for pair in range(2):
            top = value[:n, 128 * pair : 128 * pair + 128]
            bottom = value[n:, 128 * pair : 128 * pair + 128]
            first = jnp.where(low_lanes, top, pltpu.roll(bottom, 64, 1))
            second = jnp.where(low_lanes, pltpu.roll(top, 64, 1), bottom)
            for g, block in ((2 * pair, first), (2 * pair + 1, second)):
                out_ref[32 * g : 32 * g + 32, 8 * c : 8 * c + 8, :] = block.reshape(32, 8, 128)


def streamwise_backward(
    in_ref, table_ref, drift_ref, out_ref, low_ref, high_ref, up_ref, down_ref
):
    comps, local_z, local_y, count = out_ref.shape

    for c in range(comps):
        parts = []
        for part in range(2):
            chunks = [
                in_ref[pl.ds(c * 8 + part * 4 + a, count // 2, stride=24), :] for a in range(4)
            ]
            parts.append(jnp.concatenate(chunks, 1))
        value = jnp.concatenate(parts, 0).T
        result = right_product(value, table_ref[...]) + drift_ref[0, c]
        result = result.reshape(local_z, local_y, count)
        out_ref[c] = result
        up_ref[c] = result[local_z - RIM :]
        down_ref[c] = result[:RIM]
    for c in range(comps):
        for z in range(local_z):
            row = (c * local_z + z) * RIM
            low_ref[row : row + RIM, :] = out_ref[c, z, 0:RIM, :]
            high_ref[row : row + RIM, :] = out_ref[c, z, local_y - RIM : local_y, :]


def edge_kernel(above_ref, below_ref, tail_ref, up_ref, down_ref):
    comps, local_z, _, count = tail_ref.shape
    for c in range(comps):
        for z in range(local_z):
            row = (c * local_z + z) * RIM
            tail_ref[c, z, 0:RIM, :] = above_ref[row : row + RIM, :]
            tail_ref[c, z, RIM : 8 - RIM, :] = jnp.zeros((8 - 2 * RIM, count), F32)
            tail_ref[c, z, 8 - RIM : 8, :] = below_ref[row : row + RIM, :]
        up_ref[c] = tail_ref[c, local_z - RIM :]
        down_ref[c] = tail_ref[c, :RIM]


def weights(shift, small=False):
    zero = jnp.zeros_like(shift)
    if small:
        left = shift < 0
        frac = jnp.where(left, shift + 1.0, shift)
    else:
        base = jnp.floor(shift)
        frac = shift - base
    rest = 1.0 - frac
    side = -0.5 * frac * rest
    before = side * rest
    after = side * frac
    near = 1.0 + frac * frac * (1.5 * frac - 2.5)
    far = 1.0 - (before + near + after)
    if small:
        values = [zero, before, near, far, after, zero]
        return {o: jnp.where(left, values[o + 3], values[o + 2]) for o in range(-2, 3)}
    at = {k: base == k for k in range(-4, 4)}
    result = {}
    for o in range(-2, 3):
        value = jnp.where(at[o - 2], after, zero)
        value = jnp.where(at[o - 1], far, value)
        value = jnp.where(at[o], near, value)
        result[o] = jnp.where(at[o + 1], before, value)
    return result


def rotated(value, steps):
    return pltpu.roll(value, steps % value.shape[1], 1)


def inflow_kernel(
    wake_ref, speed_ref, tail_ref, low_ref, low_tail_ref, high_ref, high_tail_ref, field_ref,
    out_ref, line_ref,
):
    planes, local_z = field_ref.shape[1], speed_ref.shape[1]
    lane = lax.broadcasted_iota(jnp.int32, (72, 128), 1)

    @pl.when(wake_ref[0] == 0)
    def _():
        line_ref[...] = jnp.zeros(line_ref.shape, F32)
        columns = jnp.zeros((72, 128), F32)
        for q in range(planes + 2):
            base = 24 * (q % 5)
            for c in range(3):
                if q < RIM:
                    own, end, z = low_ref, low_tail_ref, q
                elif q < RIM + local_z:
                    own, end, z = speed_ref, tail_ref, q - RIM
                else:
                    own, end, z = high_ref, high_tail_ref, q - RIM - local_z
                first, last = [
                    jnp.concatenate([own[c, z, :, lanes], end[c, z, :, lanes]], 0)
                    for lanes in (slice(0, 128), slice(128, 256))
                ]
                at = base + 4 * c
                here = (lane >= at) & (lane < at + 4)
                ends = jnp.where(lane < 64, first, last)
                columns = jnp.where(here, rotated(ends, at + 3), columns)
                if 1 <= q <= planes:
                    at = base + 12 + 2 * c
                    here = (lane >= at) & (lane < at + 2)
                    columns = jnp.where(
                        here, rotated(field_ref[c, q - 1, :, 128:], at + 2), columns
                    )
            if q % 5 == 4 or q == planes + 1:
                gap = jnp.zeros((40, 128), F32)
                whole = jnp.concatenate([columns, columns[:8], gap, columns[64:]], 0)
                row = 120 * (q // 5)
                line_ref[row : row + 120, :] = whole.T[:120]
                columns = jnp.zeros((72, 128), F32)

        def line(row, plane):
            return line_ref[pl.ds(24 * plane + row, 16, stride=24), :]

        shift = [weights(TIME_STEP * line(x, 1)) for x in (1, 2)]
        part = [[line(12 + 2 * c + x, 1) for x in range(2)] for c in range(3)]
        for c in range(3):
            strength = []
            for x in range(2):
                row = 4 * c + 1 + x
                value = line(row, 1)
                strength.append(
                    part[c][x]
                    + (0.5 * TIME_STEP)
                    * (
                        part[0][x] * (line(row + 1, 1) - line(row - 1, 1))
                        + part[1][x] * (rotated(value, -1) - rotated(value, 1))
                        + part[2][x] * (line(row, 2) - line(row, 0))
                    )
                )
            rows = (
                strength[0] * shift[0][2] + strength[1] * shift[1][1],
                strength[1] * shift[1][2],
                line(4 * c + 2, 1),
            )
            for i in range(2):
                out_ref[pl.ds(2 * planes * c + i, planes, stride=2), :] = rows[i][:planes]
            first = 6 * planes + planes * c
            out_ref[first : first + planes, :] = rows[2][:planes]


def fill_speed(speed_ref, tail_ref, low_ref, low_tail_ref, high_ref, high_tail_ref, all_ref):
    local_z = speed_ref.shape[1]
    most = jnp.zeros((8, 128), F32)
    for c in range(3):
        for t in range(2):
            lanes = slice(128 * t, 128 * t + 128)
            for own, end, first in (
                (low_ref, low_tail_ref, 0),
                (speed_ref, tail_ref, RIM),
                (high_ref, high_tail_ref, RIM + local_z),
            ):
                planes = slice(first, first + own.shape[1])
                body = own[c, :, 0:64, lanes]
                tail = end[c, :, :, lanes]
                all_ref[c, planes, t, 8:72, :] = body
                all_ref[c, planes, t, 0:8, :] = tail
                all_ref[c, planes, t, 72:80, :] = tail
                all_ref[c, planes, t, 80:88, :] = body[:, 0:8]
                most = jnp.maximum(most, jnp.max(jnp.abs(body).reshape(-1, 8, 128), 0))
                most = jnp.maximum(most, jnp.max(jnp.abs(tail), 0))
    return jnp.max(most)


def wake_kernel(
    wake_ref, speed_ref, tail_ref, low_ref, low_tail_ref, high_ref, high_tail_ref, field_ref,
    inflow_ref, out_ref, speed_any,
    all_ref, column_ref, moved_ref, across_ref, lateral_ref, upward_ref, sem,
):
    copy = pltpu.make_async_copy(speed_ref, speed_any, sem)
    copy.start()
    planes = field_ref.shape[1]
    local_z, local_y = out_ref.shape[1], out_ref.shape[2]
    size = 72
    lane = lax.broadcasted_iota(jnp.int32, (size, 128), 1)
    is_wake = wake_ref[0] != 0
    entering_lane = is_wake & (lane == 0)
    leaving_lane = is_wake & (lane == 127)
    inflow_lanes = is_wake & (lane < 2)
    crossing = {o: is_wake & (lane >= 128 - o if o > 0 else lane < -o) for o in (-2, -1, 1, 2)}
    most = fill_speed(
        speed_ref, tail_ref, low_ref, low_tail_ref, high_ref, high_tail_ref, all_ref
    )
    missing = 128 - inflow_ref.shape[0]
    column_ref[...] = jnp.concatenate([inflow_ref[...], jnp.zeros((missing, 128), F32)], 0).T
    is_small = TIME_STEP * most < 0.999

    def turned(pair, o):
        first, second = rotated(pair[0], o), rotated(pair[1], o)
        swap = lane < o if o > 0 else lane >= 128 + o
        return jnp.where(swap, second, first), jnp.where(swap, first, second)

    def step(p, small):
        for block in range(72 // size):
            here = slice(size * block, size * block + size)
            kept = slice(8 + size * block, 8 + size * block + size)
            is_end = block == 72 // size - 1

            def velocity(c, plane, t, steps=0):
                row = 8 + size * block + steps
                return all_ref[c, plane, t, row : row + size, :]

            inflow = column_ref[here, :]
            along = []
            for t in range(2):
                along.append(weights(TIME_STEP * velocity(0, p + 1, t), small))
                across = weights(TIME_STEP * velocity(1, p + 1, t), small)
                for o in range(-2, 3):
                    across_ref[o + 2, t, kept, :] = across[o]
                    if is_end:
                        across_ref[o + 2, t, 0:8, :] = across[o][size - 8 :]
            for o in (-2, -1, 1, 2):
                t = 1 if o > 0 else 0
                along[t][o] = jnp.where(crossing[o], 0.0, along[t][o])
            part = [
                [field_ref[c, p, here, 128 * t : 128 * t + 128] for t in range(2)]
                for c in range(3)
            ]
            for c in range(3):
                value = [velocity(c, p + 1, t) for t in range(2)]
                ahead, behind = list(turned(value, -1)), list(turned(value, 1))
                entering = pltpu.roll(inflow, 128 - (6 + c) * planes - p, 1)
                behind[0] = jnp.where(entering_lane, entering, behind[0])
                ahead[1] = jnp.where(leaving_lane, value[1], ahead[1])
                strength = []
                for t in range(2):
                    strength.append(
                        part[c][t]
                        + (0.5 * TIME_STEP)
                        * (
                            part[0][t] * (ahead[t] - behind[t])
                            + part[1][t] * (velocity(c, p + 1, t, 1) - velocity(c, p + 1, t, -1))
                            + part[2][t] * (velocity(c, p + 2, t) - velocity(c, p, t))
                        )
                    )
                total = [strength[t] * along[t][0] for t in range(2)]
                passed_on = pltpu.roll(inflow, 128 - 2 * planes * c - 2 * p, 1)
                total[0] = total[0] + jnp.where(inflow_lanes, passed_on, 0.0)
                for o in (-2, -1, 1, 2):
                    pair = turned([strength[t] * along[t][o] for t in range(2)], o)
                    total = [total[t] + pair[t] for t in range(2)]
                for t in range(2):
                    moved_ref[c, t, kept, :] = total[t]
                    if is_end:
                        moved_ref[c, t, 0:8, :] = total[t][size - 8 :]
        tall = 32
        for block in range(local_y // tall):
            here = slice(tall * block, tall * block + tall)
            for t in range(2):
                total = [jnp.zeros((tall, 128), F32) for _ in range(3)]
                for o in range(-2, 3):
                    first = 8 + tall * block - o
                    weight = across_ref[o + 2, t, first : first + tall, :]
                    for c in range(3):
                        term = moved_ref[c, t, first : first + tall, :] * weight
                        total[c] = term if o == -2 else total[c] + term
                for c in range(3):
                    lateral_ref[c, p, t, here, :] = total[c]
                first = 8 + tall * block
                upward = weights(
                    TIME_STEP * all_ref[2, p + 1, t, first : first + tall, :], small
                )
                for o in range(-2, 3):
                    upward_ref[o + 2, p, t, here, :] = upward[o]

    def run(small):
        def one(p, carry):
            step(p, small)
            return carry

        lax.fori_loop(0, planes, one, 0)

    @pl.when(is_small)
    def _():
        run(True)

    @pl.when(jnp.logical_not(is_small))
    def _():
        run(False)

    def gather(z, carry):
        tall = 32
        for t in range(2):
            for block in range(local_y // tall):
                here = slice(tall * block, tall * block + tall)
                total = [None] * 3
                for o in range(-2, 3):
                    weight = upward_ref[o + 2, z + 2 - o, t, here, :]
                    for c in range(3):
                        term = lateral_ref[c, z + 2 - o, t, here, :] * weight
                        total[c] = term if o == -2 else total[c] + term
                for c in range(3):
                    out_ref[c, z, here, 128 * t : 128 * t + 128] = total[c]
        return carry

    lax.fori_loop(0, local_z, gather, 0)
    copy.wait()


def call(kernel, shapes, args, smem=(), far=(), far_out=(), scratch=(), limit=24):
    single = not isinstance(shapes, list)
    outs = [jax.ShapeDtypeStruct(s, F32) for s in ([shapes] if single else shapes)]
    def space(i):
        return pltpu.SMEM if i in smem else pltpu.HBM if i in far else pltpu.VMEM

    specs = [pl.BlockSpec(memory_space=space(i)) for i in range(len(args))]
    out = pl.pallas_call(
        kernel,
        out_shape=outs,
        in_specs=specs,
        out_specs=[
            pl.BlockSpec(memory_space=pltpu.HBM if i in far_out else pltpu.VMEM)
            for i in range(len(outs))
        ],
        scratch_shapes=list(scratch),
        compiler_params=pltpu.CompilerParams(vmem_limit_bytes=limit * 1024 * 1024),
    )(*args)
    return out[0] if single else out


def forward_lines(field):
    count = field.shape[3]
    table = jnp.asarray(forward_table(count))
    scratch = (
        pltpu.VMEM(field.shape, F32),
        pltpu.VMEM(table.shape, BF16),
        pltpu.SemaphoreType.DMA((field.shape[0] + 1,)),
    )
    shape = (count // 2 * 24, 128)
    return call(streamwise_forward, shape, (field, table), far=(0, 1), scratch=scratch, limit=61)


def solve_plane(spectrum, owner, tables):
    count = tables[3].shape[1]
    args = (owner.reshape(1), spectrum, *tables)
    scratch = [pltpu.VMEM(spectrum.shape, F32)]
    scratch += [pltpu.VMEM((3, 2 * count, count), F32), pltpu.VMEM((3, count, 2 * count), F32)]
    scratch += [pltpu.VMEM(t.shape, t.dtype) for t in tables]
    scratch += [pltpu.SemaphoreType.DMA((len(tables) + 1,))]
    far = (1, 2, 3, 4, 5)
    return call(
        plane_kernel, spectrum.shape, args, smem=(0,), far=far, scratch=scratch, limit=54
    )


def backward_lines(spectrum, drift, table, shape):
    edge = (shape[0] * shape[1] * RIM, shape[3])
    planes = (shape[0], RIM, *shape[2:])
    shapes = [shape, edge, edge, planes, planes]
    return call(streamwise_backward, shapes, (spectrum, table, drift), smem=(2,))


def edges(above, below, shape):
    comps, local_z, _, count = shape
    send = (comps, RIM, 8, count)
    return call(edge_kernel, [(comps, local_z, 8, count), send, send], (above, below))


def inflow_columns(wake, *arrays):
    planes = arrays[-1].shape[1]
    scratch = [pltpu.VMEM((24 * (planes + 6), 128), F32)]
    args = (wake, *arrays)
    return call(inflow_kernel, (9 * planes + 4, 128), args, smem=(0,), scratch=scratch)


def wake_step(wake, *arrays):
    shape = arrays[0].shape
    comps, local_z, local_y, count = shape
    lanes, planes = count // 128, local_z + 4
    scratch = [
        pltpu.VMEM((comps, planes + 2, lanes, local_y + 24, 128), F32),
        pltpu.VMEM((128, 128), F32),
        pltpu.VMEM((comps, lanes, local_y + 16, 128), F32),
        pltpu.VMEM((5, lanes, local_y + 16, 128), F32),
        pltpu.VMEM((comps, planes, lanes, local_y, 128), F32),
        pltpu.VMEM((5, planes, lanes, local_y, 128), F32),
        pltpu.SemaphoreType.DMA,
    ]
    args = (wake, *arrays)
    return call(wake_kernel, [shape, shape], args, smem=(0,), far_out=(1,), scratch=scratch)


def from_before(value, axis):
    count = lax.axis_size(axis)
    return lax.ppermute(value, axis, [(i, (i + 1) % count) for i in range(count)])


def from_after(value, axis):
    count = lax.axis_size(axis)
    return lax.ppermute(value, axis, [((i + 1) % count, i) for i in range(count)])


def wider_rows(field):
    above = from_after(field[:, :, :2], "gy")
    below = from_before(field[:, :, field.shape[2] - 2 :], "gy")
    above = jnp.pad(above, ((0, 0), (0, 0), (0, 4), (0, 0)))
    return jnp.concatenate([field, above, below], 2)


def wider_planes(field):
    low = from_before(field[:, field.shape[1] - 2 :], "gz")
    high = from_after(field[:, :2], "gz")
    return jnp.concatenate([low, field, high], 1)


def body(vorticity, wind):
    wake = (lax.axis_index("grp") == 1).astype(jnp.int32).reshape(1)
    field = vorticity[0]
    count_x = field.shape[3]
    size_gz = lax.axis_size("gz")
    groups = lax.axis_size("gy") * size_gz
    owner = lax.axis_index("gy") * size_gz + lax.axis_index("gz")
    axes = ("gy", "gz")
    spectrum = forward_lines(field)
    start = lax.axis_index("grp") * 0
    spectrum, start, halo_field, wake = lax.optimization_barrier((spectrum, start, field, wake))
    spectrum = spectrum.reshape(groups, 24, 128)
    spectrum = lax.all_to_all(spectrum, axes, split_axis=0, concat_axis=0, tiled=True)
    wide = wider_rows(halo_field)
    tables, streamwise = run_time_tables(start, count_x, size_gz)
    spectrum, wide, tables, streamwise = lax.optimization_barrier(
        (spectrum, wide, tables, streamwise)
    )
    spectrum = solve_plane(spectrum, owner, tables)
    spectrum, wide = lax.optimization_barrier((spectrum, wide))
    spectrum = lax.all_to_all(spectrum, axes, split_axis=0, concat_axis=0, tiled=True)
    wide = wider_planes(wide)
    spectrum, wide = lax.optimization_barrier((spectrum, wide))
    spectrum = spectrum.reshape(groups * 24, 128)
    speed, first, last, up, down = backward_lines(spectrum, wind, streamwise, field.shape)
    above, below = from_after(first, "gy"), from_before(last, "gy")
    low, high = from_before(up, "gz"), from_after(down, "gz")
    tail, up_tail, down_tail = edges(above, below, speed.shape)
    low_tail, high_tail = from_before(up_tail, "gz"), from_after(down_tail, "gz")
    arrays = (speed, tail, low, low_tail, high, high_tail, wide)
    inflow = lax.ppermute(inflow_columns(wake, *arrays), "grp", [(0, 1)])
    result, velocity = wake_step(wake, *arrays, inflow)
    return (result[None], velocity[None])


def solution(mesh):
    return jax.shard_map(
        body,
        mesh=mesh,
        in_specs=(P("grp", None, "gz", "gy", None), P("grp", None)),
        out_specs=(P("grp", None, "gz", "gy", None), P("grp", None, "gz", "gy", None)),
        check_vma=False,
    )
```
